128 devices in a mesh: dp: 8 (over y_lo, z), expert: 16 (over y_hi, x, core).
Axes of the slice: x: 4, y: 4 (y_hi: 2, y_lo: 2; y = y_hi * 2 + y_lo), z: 4, core: 2. Of those that a mesh axis runs over, the one named last changes fastest.
Arguments:
- tokens: bfloat16 [256, 768, 1024], P(None, ('dp', 'expert')), may hold values from -200 to 200
- grad_out: bfloat16 [256, 768, 1024], P(None, ('dp', 'expert')), may hold values from -6 to 6
- slot_out: bfloat16 [512, 768, 1024], P('expert', 'dp'), may hold values from -6 to 6
- slot_params: bfloat16 [512, 1024], P('expert'), may hold values from -2 to 2
Outputs:
- grad_tokens: bfloat16 [256, 768, 1024], P(None, ('dp', 'expert'))
- grad_slot_out: bfloat16 [512, 768, 1024], P('expert', 'dp')
- grad_params: float32 [512, 1024], P('expert', 'dp')
The draws below stay inside these ranges and needn't reach their ends.
All inputs are finite; a program needn't handle non-finite values.
Results may differ from the reference program's by a relative error of at most 0.018.
Values may be sent and summed in bfloat16 or wider, within the bound.
A program may use at most 128 MiB of HBM per device.

```python
import math
import jax
import jax.numpy as jnp

D = 1024
SLOTS = 512
PATCHES = 256
IMAGES = 768


def slot_table(key):
    inner = jax.random.fold_in(key, 11)
    spread = 2.0 / math.sqrt(D)
    values = jnp.clip(jax.random.normal(inner, (SLOTS, D)) * spread, -6.0 * spread, 6.0 * spread)
    return values.astype(jnp.bfloat16).astype(jnp.float32)


def draw_slot_params(key, part):
    return slot_table(key).astype(jnp.bfloat16)


def draw_tokens(key, part):
    key_base = jax.random.fold_in(jax.random.fold_in(key, 23), 0)
    values = jnp.clip(jax.random.normal(key_base, (PATCHES, IMAGES, D)), -6.0, 6.0)
    return values.astype(jnp.bfloat16)


def block_levels(own_key, dims, pieces, smallest, largest):
    level, own = 1.0, jax.random.fold_in(own_key, 6)
    for axis_at, parts in pieces:
        steps = jnp.exp(jax.random.uniform(jax.random.fold_in(own, axis_at), (parts,), jnp.float32, smallest / len(pieces), largest / len(pieces)))
        level = level * jnp.repeat(steps, dims[axis_at] // parts).reshape([-1 if axis == axis_at else 1 for axis in range(len(dims))])
    return level


def gaussian(rng, dims, width, reach, cuts=(), kind=jnp.bfloat16):
    loudness = block_levels(rng, dims, cuts, -0.22, 0.18) if cuts else 1.0
    drawn = jax.random.normal(rng, dims, jnp.float32) * width * loudness
    return jnp.minimum(jnp.maximum(drawn, -reach), reach).astype(kind)


def setup_inputs(seed: int = 0) -> dict:
    key_of = jax.random.split(jax.random.key(seed), 5)
    return {
        "tokens": draw_tokens(jax.random.fold_in(key_of[4], 71), 0),
        "grad_out": gaussian(key_of[1], (PATCHES, IMAGES, D), 1.0, 6.0, ((1, 128),)),
        "slot_out": gaussian(key_of[2], (SLOTS, IMAGES, D), 1.0, 6.0, ((0, 16), (1, 8))),
        "slot_params": draw_slot_params(jax.random.fold_in(key_of[4], 71), 0),
    }


def reference(tokens, grad_out, slot_out, slot_params):
    tok_wide = tokens.astype(jnp.float32)
    grad_wide = grad_out.astype(jnp.float32)
    param_wide = slot_params.astype(jnp.float32)
    logits = jnp.einsum('tbd,sd->tbs', tok_wide, param_wide)
    combine = jax.nn.softmax(logits, axis=-1)
    combine_low = combine.astype(jnp.bfloat16)
    grad_slot = jnp.einsum('tbs,tbd->sbd', combine_low.astype(jnp.float32), grad_wide).astype(jnp.bfloat16)
    grad_comb = jnp.einsum('tbd,sbd->tbs', grad_wide, slot_out.astype(jnp.float32))
    rowdot = jnp.sum(combine * grad_comb, axis=-1, keepdims=True)
    grad_logits = (combine * (grad_comb - rowdot)).astype(jnp.bfloat16)
    logit_wide = grad_logits.astype(jnp.float32)
    grad_tok = jnp.einsum('tbs,sd->tbd', logit_wide, param_wide).astype(jnp.bfloat16)
    grad_params = jnp.einsum('tbs,tbd->sd', logit_wide, tok_wide)
    return grad_tok, grad_slot, grad_params
```

```python
import functools

import jax
import jax.numpy as jnp
from jax import lax
from jax.experimental import pallas as pl
from jax.experimental.pallas import tpu as pltpu
from jax.sharding import PartitionSpec as P

MESH = pl.DeviceIdType.MESH
BF = jnp.bfloat16
F32 = jnp.float32

ROWS, XS, CORES = 2, 4, 2
NEAR, ZS = 2, 4
CHIPS = ROWS * XS
STEPS = ((1, 0), (1, 2), (0, 1), (0, 3), (1, 1), (1, 3), (0, 2))
ORDER = tuple((r, x, c) for c in range(CORES) for r, x in STEPS) + ((0, 0, 1),)
NT = (((1,), (1,)), ((), ()))
TN = (((0,), (0,)), ((), ()))


def dot(a, b, dims):
    return lax.dot_general(a, b, dims, preferred_element_type=F32)


def row_order(own, lanes, flip):
    n = own * lanes
    r = lax.broadcasted_iota(jnp.int32, (n, n), 0)
    c = lax.broadcasted_iota(jnp.int32, (n, n), 1)
    if flip:
        hit = c == (r % lanes) * own + r // lanes
    else:
        hit = c == (r % own) * lanes + r // own
    return jnp.where(hit, 1.0, 0.0).astype(BF)


def exchange(
    tok_hbm, go_hbm, so_hbm, sp_hbm,
    gso, gt, gp,
    tok, go, raw, send_a, recv_a, send_b, par, comb, pp, perm,
    r1s, r1r, acc, r2s, r2r, r3s, r3r, r4s, r4r,
    so_sem, in_sem, par_s, par_r, as_sem, ar_sem, bs_sem, br_sem, own_sem, red_s, red_r,
):
    imgs, width = tok.shape[0], tok.shape[2]
    blocks, own, lanes = raw.shape[0], so_hbm.shape[0], so_hbm.shape[2]
    slots = CHIPS * CORES * own
    tokens = tok.shape[1]
    d = lax.axis_index("dp")
    e = lax.axis_index("expert")
    row, x, c = e // (XS * CORES), (e // CORES) % XS, e % CORES
    chip = e // CORES
    near, z = d // ZS, d % ZS

    def peer(dr, dx, dc):
        return ((row + dr) % ROWS) * (XS * CORES) + ((x + dx) % XS) * CORES + (c + dc) % CORES

    def zpeer(k):
        return (near * ZS + (z + k) % ZS, e)

    side = ((1 - near) * ZS + z, e)
    partner = (d, peer(0, 0, 1))

    barrier = pltpu.get_barrier_semaphore()
    others = [(d, peer(*o)) for o in ORDER] + [zpeer(k) for k in range(1, ZS)] + [side]
    for dev in others:
        pl.semaphore_signal(barrier, inc=1, device_id=dev, device_id_type=MESH)

    def load_so(g):
        return pltpu.make_async_copy(so_hbm.at[:, g], raw.at[g], so_sem.at[g])

    sp_in = pltpu.make_async_copy(sp_hbm.at[z], par.at[chip, c, z], in_sem.at[0])
    tok_in = pltpu.make_async_copy(tok_hbm, tok, in_sem.at[1])
    go_in = pltpu.make_async_copy(go_hbm, go, in_sem.at[2])
    sp_in.start()
    for g in range(blocks):
        load_so(g).start()
    tok_in.start()
    go_in.start()
    perm[...] = row_order(own, lanes, False)

    pl.semaphore_wait(barrier, len(others))

    def remote(src, dst, s, r, dev):
        return pltpu.make_async_remote_copy(
            src_ref=src, dst_ref=dst, send_sem=s, recv_sem=r, device_id=dev, device_id_type=MESH
        )

    def par_row(i):
        r, dx = STEPS[i]
        piece = par.at[chip, c, z]
        return remote(piece, piece, par_s.at[i], par_r.at[i], (d, peer(r, dx, 0)))

    def par_z(k):
        piece = par.at[:, c, z]
        n = len(STEPS) + k - 1
        return remote(piece, piece, par_s.at[n], par_r.at[n], zpeer(k))

    def par_core():
        piece = par.at[:, c]
        n = len(STEPS) + ZS - 1
        return remote(piece, piece, par_s.at[n], par_r.at[n], partner)

    sp_in.wait()
    for i in range(len(STEPS)):
        par_row(i).start()

    @pl.loop(0, blocks)
    def _(g):
        load_so(g).wait()
        block = raw.at[g].reshape(own * lanes, width)
        out = send_a.at[pl.ds(g * lanes, lanes)].reshape(own * lanes, width)
        for n in range(0, width, 256):
            out[:, n : n + 256] = dot(perm[...], block[:, n : n + 256], (((1,), (0,)), ((), ()))).astype(BF)

    def send_out(j, o):
        p = peer(*o)
        return remote(
            send_a.at[p * imgs + j], recv_a.at[j, e], as_sem.at[j], ar_sem.at[j], (d, p)
        )

    def keep_out(j):
        return pltpu.make_async_copy(send_a.at[e * imgs + j], recv_a.at[j, e], own_sem.at[0, j])

    def send_back(j, o):
        p = peer(*o)
        return remote(
            send_b.at[j, p], gso.at[e * imgs + j], bs_sem.at[j], br_sem.at[j], (d, p)
        )

    def keep_back(j):
        return pltpu.make_async_copy(send_b.at[j, e], gso.at[e * imgs + j], own_sem.at[1, j])

    @pl.loop(0, imgs)
    def _(j):
        for o in ORDER:
            send_out(j, o).start()
        keep_out(j).start()

    for i in range(len(STEPS)):
        par_row(i).wait_recv()
    for k in range(1, ZS):
        par_z(k).start()
    for k in range(1, ZS):
        par_z(k).wait_recv()
    par_core().start()
    par_core().wait_recv()
    tok_in.wait()
    go_in.wait()

    params = par.reshape(slots, width)

    @pl.loop(0, imgs)
    def _(j):
        logits = dot(params[...], tok[j], NT)
        top = jnp.max(logits, axis=0, keepdims=True)
        raised = jnp.exp(logits - top)
        weight = raised / jnp.sum(raised, axis=0, keepdims=True)
        comb[j] = weight
        low = weight.astype(BF)
        out = send_b.at[j].reshape(slots, width)
        for n in range(0, width, 256):
            out[:, n : n + 256] = dot(low, go[j, :, n : n + 256], (((1,), (0,)), ((), ()))).astype(BF)

        @pl.when(j > 0)
        def _():
            for o in ORDER:
                send_back(j - 1, o).start()
            keep_back(j - 1).start()

    pp[...] = jnp.zeros_like(pp)
    for o in ORDER:
        send_back(imgs - 1, o).start()
    keep_back(imgs - 1).start()

    def all_of(ref, sem):
        return pltpu.make_async_copy(ref, ref, sem)

    @pl.loop(0, imgs)
    def _(j):
        all_of(recv_a.at[j, pl.ds(0, len(ORDER))], ar_sem.at[j]).wait()
        keep_out(j).wait()
        rows = recv_a.at[j].reshape(slots, width)
        grad = dot(rows[...], go[j], NT)
        weight = comb[j]
        rowdot = jnp.sum(weight * grad, axis=0, keepdims=True)
        low = (weight * (grad - rowdot)).astype(BF)
        for n in range(0, width, 256):
            pp[:, n : n + 256] += dot(low, tok[j, :, n : n + 256], (((1,), (0,)), ((), ())))
            gt[j, :, n : n + 256] = dot(low, params[:, n : n + 256], TN).astype(BF)

    share = pp.reshape(CHIPS, CORES, own, width)
    r1s[...] = share[:, 1 - c].astype(BF)
    over_core = remote(r1s, r1r, red_s.at[0], red_r.at[0], partner)
    over_core.start()
    over_core.wait_recv()
    half = (share[:, c] + r1r[...].astype(F32)).reshape(CHIPS * own, width)
    piece = width // (NEAR * ZS)
    for n in range(NEAR):
        for k in range(ZS):
            m = (n * ZS + k) * piece
            acc[k, n] = half[:, m : m + piece]
    r2s[...] = acc[...].astype(BF)

    def over_z(k):
        return remote(r2s.at[(z + k) % ZS], r2r.at[k - 1], red_s.at[k], red_r.at[k], zpeer(k))

    for k in range(1, ZS):
        over_z(k).start()
    total = acc[z]
    for k in range(1, ZS):
        over_z(k).wait_recv()
        total = total + r2r[k - 1].astype(F32)
    acc[0] = total
    r3s[...] = acc[0, 1 - near].astype(BF)
    over_side = remote(r3s, r3r, red_s.at[ZS], red_r.at[ZS], side)
    over_side.start()
    over_side.wait_recv()
    mine = (acc[0, near] + r3r[...].astype(F32)).reshape(CHIPS, own, piece)
    r4s[...] = mine.astype(BF)
    acc[1, 0] = mine.reshape(CHIPS * own, piece)

    def over_chips(i):
        p = peer(*STEPS[i], 0)
        return remote(r4s.at[p // CORES], r4r.at[i], red_s.at[ZS + 1 + i], red_r.at[ZS + 1 + i], (d, p))

    for i in range(len(STEPS)):
        over_chips(i).start()
    owned = acc.at[1, 0].reshape(CHIPS, own, piece)[chip]
    for i in range(len(STEPS)):
        over_chips(i).wait_recv()
        owned = owned + r4r[i].astype(F32)
    gp[...] = owned

    for i in range(len(STEPS)):
        par_row(i).wait_send()
        over_chips(i).wait_send()
    for k in range(1, ZS):
        par_z(k).wait_send()
        over_z(k).wait_send()
    par_core().wait_send()
    over_core.wait_send()
    over_side.wait_send()

    @pl.loop(0, imgs)
    def _(j):
        all_of(send_a.at[pl.ds(0, len(ORDER))], as_sem.at[j]).wait()
        all_of(send_b.at[j, pl.ds(0, len(ORDER))], bs_sem.at[j]).wait()
        keep_back(j).wait()
        all_of(gso.at[pl.ds(0, len(ORDER))], br_sem.at[j]).wait()


def settle(gso, gt, gp, gso_out, gt_out, gp_out, perm, stage, sems):
    lanes, own = gso_out.shape[2], gso_out.shape[0]
    width = gso_out.shape[3]
    blocks = gso_out.shape[1]
    gt_copy = pltpu.make_async_copy(gt, gt_out, sems.at[0])
    gp_copy = pltpu.make_async_copy(gp, gp_out, sems.at[1])
    gt_copy.start()
    gp_copy.start()
    perm[...] = row_order(own, lanes, True)

    def put(g):
        return pltpu.make_async_copy(stage.at[g], gso_out.at[:, g], sems.at[2 + g])

    @pl.loop(0, blocks)
    def _(g):
        block = gso.at[pl.ds(g * lanes, lanes)].reshape(own * lanes, width)
        out = stage.at[g].reshape(own * lanes, width)
        for n in range(0, width, 256):
            out[:, n : n + 256] = dot(perm[...], block[:, n : n + 256], (((1,), (0,)), ((), ()))).astype(BF)
        put(g).start()

    @pl.loop(0, blocks)
    def _(g):
        put(g).wait()

    gt_copy.wait()
    gp_copy.wait()


def per_device(tokens, grad_out, slot_out, slot_params):
    toks, imgs, width = tokens.shape
    own, all_imgs, _ = slot_out.shape
    lanes = 8
    blocks = all_imgs // lanes
    slots = CHIPS * CORES * own
    tok = jnp.swapaxes(tokens, 0, 1)
    go = jnp.swapaxes(grad_out, 0, 1)
    so = slot_out.reshape(own, blocks, lanes, width)
    sp = slot_params.reshape(ZS, own // ZS, width)
    piece = width // (NEAR * ZS)
    anywhere = pl.BlockSpec(memory_space=pl.ANY)
    vmem = pl.BlockSpec(memory_space=pltpu.VMEM)
    dma = pltpu.SemaphoreType.DMA
    peers = len(ORDER)
    gso, gt, gp = pl.pallas_call(
        exchange,
        out_shape=(
            pltpu.VMEM((all_imgs, own, width), BF),
            pltpu.VMEM((imgs, toks, width), BF),
            pltpu.VMEM((own, piece), F32),
        ),
        in_specs=[anywhere] * 4,
        out_specs=(vmem, vmem, vmem),
        scratch_shapes=[
            pltpu.VMEM((imgs, toks, width), BF),
            pltpu.VMEM((imgs, toks, width), BF),
            pltpu.VMEM((blocks, own, lanes, width), BF),
            pltpu.VMEM((all_imgs, own, width), BF),
            pltpu.VMEM((imgs, CHIPS * CORES, own, width), BF),
            pltpu.VMEM((imgs, CHIPS * CORES, own, width), BF),
            pltpu.VMEM((CHIPS, CORES, ZS, own // ZS, width), BF),
            pltpu.VMEM((imgs, slots, toks), F32),
            pltpu.VMEM((slots, width), F32),
            pltpu.VMEM((own * lanes, own * lanes), BF),
            pltpu.VMEM((CHIPS, own, width), BF),
            pltpu.VMEM((CHIPS, own, width), BF),
            pltpu.VMEM((ZS, NEAR, CHIPS * own, piece), F32),
            pltpu.VMEM((ZS, NEAR, CHIPS * own, piece), BF),
            pltpu.VMEM((ZS - 1, NEAR, CHIPS * own, piece), BF),
            pltpu.VMEM((CHIPS * own, piece), BF),
            pltpu.VMEM((CHIPS * own, piece), BF),
            pltpu.VMEM((CHIPS, own, piece), BF),
            pltpu.VMEM((CHIPS - 1, own, piece), BF),
            dma((blocks,)),
            dma((3,)),
            dma((CHIPS + ZS - 1,)),
            dma((CHIPS + ZS - 1,)),
            dma((imgs,)),
            dma((imgs,)),
            dma((imgs,)),
            dma((imgs,)),
            dma((2, imgs)),
            dma((ZS + CHIPS,)),
            dma((ZS + CHIPS,)),
        ],
        compiler_params=pltpu.CompilerParams(
            collective_id=0, has_side_effects=True, vmem_limit_bytes=52 * 2**20
        ),
        name="exchange",
    )(tok, go, so, sp)
    gso_out, gt_out, gp_out = pl.pallas_call(
        settle,
        out_shape=(
            jax.ShapeDtypeStruct((own, blocks, lanes, width), BF),
            jax.ShapeDtypeStruct((imgs, toks, width), BF),
            jax.ShapeDtypeStruct((own, piece), F32),
        ),
        in_specs=[vmem] * 3,
        out_specs=(anywhere,) * 3,
        scratch_shapes=[
            pltpu.VMEM((own * lanes, own * lanes), BF),
            pltpu.VMEM((blocks, own, lanes, width), BF),
            dma((2 + blocks,)),
        ],
        compiler_params=pltpu.CompilerParams(vmem_limit_bytes=20 * 2**20),
        name="settle",
    )(gso, gt, gp)
    return (
        jnp.swapaxes(gt_out, 0, 1),
        gso_out.reshape(own, all_imgs, width),
        gp_out,
    )


def solution(mesh):
    return jax.shard_map(
        per_device,
        mesh=mesh,
        in_specs=(
            P(None, ("dp", "expert"), None),
            P(None, ("dp", "expert"), None),
            P("expert", "dp", None),
            P("expert", None),
        ),
        out_specs=(P(None, ("dp", "expert"), None), P("expert", "dp", None), P("expert", "dp")),
        check_vma=False,
    )
```

```python
import functools

import jax
import jax.numpy as jnp
from jax import lax
from jax.experimental import pallas as pl
from jax.experimental.pallas import tpu as pltpu
from jax.sharding import PartitionSpec as P

MESH = pl.DeviceIdType.MESH
BF = jnp.bfloat16
F32 = jnp.float32

ROWS, XS, CORES = 2, 4, 2
NEAR, ZS = 2, 4
CHIPS = ROWS * XS
STEPS = ((1, 0), (1, 2), (0, 1), (0, 3), (1, 1), (1, 3), (0, 2))
ORDER = tuple((r, x, c) for c in range(CORES) for r, x in STEPS) + ((0, 0, 1),)
NT = (((1,), (1,)), ((), ()))
TN = (((0,), (0,)), ((), ()))
NN = (((1,), (0,)), ((), ()))
KINDS = (0, 1, 2)
HELPER = ((1, 0), (0, 1), (0, 3))
PARTS = (
    (((0, 0), (0, 1), (0, 2), (0, 3)), ((0, 0), (1, 0), (0, 3), (1, 3)), ((0, 0), (1, 0), (0, 1), (1, 1))),
    (((0, 0), (0, 1), (0, 2), (0, 3)), ((0, 0), (1, 0), (0, 1), (1, 1)), ((0, 0), (1, 0), (0, 3), (1, 3))),
)
PIECES = 4
MIX = tuple(kind * 8 + k * CORES + dc for dc in range(CORES) for k in (3, 1, 2, 0) for kind in (0, 1))
BACK = tuple(tuple(tuple((k, of[k]) for k in (3, 1, 2, 0)) for of in kind) for kind in PARTS)


def back(at):
    return ((ROWS - at[0]) % ROWS, (XS - at[1]) % XS)


def add(a, b):
    return ((a[0] + b[0]) % ROWS, (a[1] + b[1]) % XS)


def dot(a, b, dims):
    return lax.dot_general(a, b, dims, preferred_element_type=F32)


def row_order(own, lanes, flip):
    n = own * lanes
    r = lax.broadcasted_iota(jnp.int32, (n, n), 0)
    c = lax.broadcasted_iota(jnp.int32, (n, n), 1)
    if flip:
        hit = c == (r % lanes) * own + r // lanes
    else:
        hit = c == (r % own) * lanes + r // own
    return jnp.where(hit, 1.0, 0.0).astype(BF)


def exchange(
    tok_hbm, go_hbm, so_hbm, sp_hbm,
    gso, gt, gp,
    tok, go, raw, send_a, slot_in, send_b, par, comb, low_w, low_s, gc_s, gc_r, gc_all, pp, perm,
    r1s, r1r, acc, r2s, r2r, r3s, r3r, r4s, r4r,
    so_sem, in_sem, par_s, par_r, go_s, go_r, as_sem, ar_sem, bs_sem, br_sem,
    low_ss, low_rs, gc_ss, gc_rs, own_sem, red_s, red_r,
):
    imgs, width, tokens = tok.shape[0], tok.shape[2], tok.shape[1]
    blocks, own, lanes = raw.shape[0], so_hbm.shape[0], so_hbm.shape[2]
    slots = CHIPS * CORES * own
    half = slots // 2
    rounds = imgs // len(KINDS)
    d = lax.axis_index("dp")
    e = lax.axis_index("expert")
    row, x, c = e // (XS * CORES), (e // CORES) % XS, e % CORES
    chip = e // CORES
    near, z = d // ZS, d % ZS

    def chip_at(dr, dx):
        return ((row + dr) % ROWS) * XS + (x + dx) % XS

    def peer(dr, dx, dc):
        return chip_at(dr, dx) * CORES + (c + dc) % CORES

    def zpeer(k):
        return (near * ZS + (z + k) % ZS, e)

    side = ((1 - near) * ZS + z, e)
    partner = (d, peer(0, 0, 1))

    barrier = pltpu.get_barrier_semaphore()
    others = [(d, peer(*o)) for o in ORDER] + [zpeer(k) for k in range(1, ZS)] + [side]
    for dev in others:
        pl.semaphore_signal(barrier, inc=1, device_id=dev, device_id_type=MESH)

    def load_so(g):
        return pltpu.make_async_copy(so_hbm.at[:, g], raw.at[g], so_sem.at[g])

    sp_in = pltpu.make_async_copy(sp_hbm.at[z], par.at[chip, c, z], in_sem.at[0])
    go_in = pltpu.make_async_copy(go_hbm, go.at[pl.ds(0, imgs)], in_sem.at[1])
    tok_in = pltpu.make_async_copy(tok_hbm, tok, in_sem.at[2])
    sp_in.start()
    go_in.start()
    for g in range(blocks):
        load_so(g).start()
    tok_in.start()
    perm[...] = row_order(own, lanes, False)

    pl.semaphore_wait(barrier, len(others))

    def remote(src, dst, s, r, dev):
        return pltpu.make_async_remote_copy(
            src_ref=src, dst_ref=dst, send_sem=s, recv_sem=r, device_id=dev, device_id_type=MESH
        )

    def all_of(ref, sem):
        return pltpu.make_async_copy(ref, ref, sem)

    def par_row(i):
        r, dx = STEPS[i]
        piece = par.at[chip, c, z]
        return remote(piece, piece, par_s.at[i], par_r.at[i], (d, peer(r, dx, 0)))

    def par_z(k):
        piece = par.at[:, c, z]
        n = len(STEPS) + k - 1
        return remote(piece, piece, par_s.at[n], par_r.at[n], zpeer(k))

    def par_core():
        piece = par.at[:, c]
        n = len(STEPS) + ZS - 1
        return remote(piece, piece, par_s.at[n], par_r.at[n], partner)

    sp_in.wait()
    for i in range(len(STEPS)):
        par_row(i).start()

    def helper(t):
        return (d, peer(*HELPER[t], 0))

    def home(t):
        return (d, peer(*back(HELPER[t]), 0))

    go_in.wait()
    step = tokens // PIECES
    for q in range(PIECES):
        for j in range(imgs):
            rows = pl.ds(q * step, step)
            remote(
                go.at[j, rows], go.at[imgs + j, rows], go_s.at[j], go_r.at[j], helper(j % len(KINDS))
            ).start()

    @pl.loop(0, blocks)
    def _(g):
        load_so(g).wait()
        block = raw.at[g].reshape(own * lanes, width)
        out = send_a.at[pl.ds(g * lanes, lanes)].reshape(own * lanes, width)
        for n in range(0, width, 256):
            out[:, n : n + 256] = dot(perm[...], block[:, n : n + 256], NN).astype(BF)

    def out_moves(j, t):
        for kind in range(2):
            for k, (dr, dx) in enumerate(PARTS[kind][t]):
                for dc in range(CORES):
                    at = back((dr, dx))
                    hr, hx = at if kind == 0 else add(at, back(HELPER[t]))
                    image = peer(hr, hx, dc) * imgs + j
                    yield kind, k, (*at, dc), send_a.at[image], slot_in.at[kind * imgs + j, k, c]

    def send_out(j, t):
        moves = list(out_moves(j, t))
        for i in MIX:
            kind, _, o, src, dst = moves[i]
            w = kind * imgs + j
            if o == (0, 0, 0):
                pltpu.make_async_copy(src, dst, own_sem.at[w]).start()
            else:
                remote(src, dst, as_sem.at[j], ar_sem.at[w], (d, peer(*o))).start()

    def wait_out(w):
        all_of(slot_in.at[w].reshape(2 * len(PARTS[0][0]), own, width).at[pl.ds(0, 7)], ar_sem.at[w]).wait()
        all_of(send_a.at[0], own_sem.at[w]).wait()

    def send_back(kind, j, t):
        hr, hx = (0, 0) if kind == 0 else back(HELPER[t])
        image = peer(hr, hx, 0) * imgs + j
        w = kind * imgs + j
        for k, (dr, dx) in BACK[kind][t]:
            for dc in range(CORES):
                src, dst = send_b.at[w, k, (c + dc) % CORES], gso.at[image]
                if (dr, dx, dc) == (0, 0, 0):
                    pltpu.make_async_copy(src, dst, own_sem.at[2 * imgs + w]).start()
                else:
                    remote(src, dst, bs_sem.at[w], br_sem.at[w], (d, peer(dr, dx, dc))).start()

    for t in range(len(KINDS)):
        send_out(t, t)

    for i in range(len(STEPS)):
        par_row(i).wait_recv()
    for k in range(1, ZS):
        par_z(k).start()
    for k in range(1, ZS):
        par_z(k).wait_recv()
    par_core().start()
    par_core().wait_recv()
    tok_in.wait()

    params = par.reshape(slots, width)

    def part_chips(kind, t):
        at = (0, 0) if kind == 0 else HELPER[t]
        return [chip_at(*add(at, p)) for p in PARTS[kind][t]]

    def send_low(j, t):
        return remote(low_s.at[j], low_w.at[imgs + j], low_ss.at[j], low_rs.at[j], helper(t))

    @pl.loop(0, rounds)
    def _(r):
        for t in range(len(KINDS)):
            j = r * len(KINDS) + t
            logits = dot(params[...], tok[j], NT)
            top = jnp.max(logits, axis=0, keepdims=True)
            raised = jnp.exp(logits - top)
            weight = raised / jnp.sum(raised, axis=0, keepdims=True)
            comb[j] = weight.reshape(CHIPS, CORES * own, tokens)
            for k, p in enumerate(part_chips(0, t)):
                low_w[j, k] = comb[j, p].astype(BF)
            for k, p in enumerate(part_chips(1, t)):
                low_s[j, k] = comb[j, p].astype(BF)
            if t > 0:
                send_low(j - 1, t - 1).start()
        send_low(r * len(KINDS) + len(KINDS) - 1, len(KINDS) - 1).start()

    for t in range(len(KINDS)):
        send_out(len(KINDS) + t, t)

    def slot_grads(w):
        low = low_w[w].reshape(half, tokens)
        out = send_b.at[w].reshape(half, width)
        for n in range(0, width, 256):
            out[:, n : n + 256] = dot(low, go[w, :, n : n + 256], NN).astype(BF)

    @pl.loop(0, imgs)
    def _(j):
        slot_grads(j)

    for t in range(len(KINDS)):
        send_back(0, t, t)

    @pl.loop(0, imgs)
    def _(j):
        all_of(low_w.at[imgs + j], low_rs.at[j]).wait()
        all_of(go.at[imgs + j], go_r.at[j]).wait()
        slot_grads(imgs + j)

    def logit_dot(w):
        return dot(slot_in[w].reshape(half, width), go[w], NT).reshape(-1, CORES * own, tokens)

    def send_gc(j, t):
        return remote(gc_s.at[j], gc_r.at[j], gc_ss.at[j], gc_rs.at[j], home(t))

    @pl.loop(0, rounds)
    def _(r):
        for t in range(len(KINDS)):
            j = r * len(KINDS) + t
            wait_out(imgs + j)
            gc_s[j] = logit_dot(imgs + j).astype(BF)
            if t > 0:
                send_gc(j - 1, t - 1).start()
        send_gc(r * len(KINDS) + len(KINDS) - 1, len(KINDS) - 1).start()

    pp[...] = jnp.zeros_like(pp)
    for t in range(len(KINDS)):
        send_back(0, len(KINDS) + t, t)
    for t in range(len(KINDS)):
        send_back(1, t, t)

    @pl.loop(0, rounds)
    def _(r):
        for t in range(len(KINDS)):
            j = r * len(KINDS) + t
            wait_out(j)
            part = logit_dot(j)
            for k, p in enumerate(part_chips(0, t)):
                gc_all[p] = part[k]
            send_gc(j, t).wait_recv()
            for k, p in enumerate(part_chips(1, t)):
                gc_all[p] = gc_r[j, k].astype(F32)
            grad = gc_all[...].reshape(slots, tokens)
            weight = comb[j].reshape(slots, tokens)
            rowdot = jnp.sum(weight * grad, axis=0, keepdims=True)
            low = (weight * (grad - rowdot)).astype(BF)
            for n in range(0, width, 256):
                pp[:, n : n + 256] += dot(low, tok[j, :, n : n + 256], NN)
                gt[j, :, n : n + 256] = dot(low, params[:, n : n + 256], TN).astype(BF)

    share = pp.reshape(CHIPS, CORES, own, width)
    r1s[...] = share[:, 1 - c].astype(BF)
    over_core = remote(r1s, r1r, red_s.at[0], red_r.at[0], partner)
    over_core.start()
    send_back(1, len(KINDS), 0)
    over_core.wait_recv()
    both = (share[:, c] + r1r[...].astype(F32)).reshape(CHIPS * own, width)
    piece = width // (NEAR * ZS)
    for n in range(NEAR):
        for k in range(ZS):
            m = (n * ZS + k) * piece
            acc[k, n] = both[:, m : m + piece]
    r2s[...] = acc[...].astype(BF)

    def over_z(k):
        return remote(r2s.at[(z + k) % ZS], r2r.at[k - 1], red_s.at[k], red_r.at[k], zpeer(k))

    for k in range(1, ZS):
        over_z(k).start()
    total = acc[z]
    for k in range(1, ZS):
        over_z(k).wait_recv()
        total = total + r2r[k - 1].astype(F32)
    acc[0] = total
    r3s[...] = acc[0, 1 - near].astype(BF)
    over_side = remote(r3s, r3r, red_s.at[ZS], red_r.at[ZS], side)
    over_side.start()
    send_back(1, len(KINDS) + 1, 1)
    over_side.wait_recv()
    mine = (acc[0, near] + r3r[...].astype(F32)).reshape(CHIPS, own, piece)
    r4s[...] = mine.astype(BF)
    acc[1, 0] = mine.reshape(CHIPS * own, piece)

    def over_chips(i):
        p = peer(*STEPS[i], 0)
        return remote(r4s.at[p // CORES], r4r.at[i], red_s.at[ZS + 1 + i], red_r.at[ZS + 1 + i], (d, p))

    for i in range(len(STEPS)):
        over_chips(i).start()
    send_back(1, len(KINDS) + 2, 2)
    owned = acc.at[1, 0].reshape(CHIPS, own, piece)[chip]
    for i in range(len(STEPS)):
        over_chips(i).wait_recv()
        owned = owned + r4r[i].astype(F32)
    gp[...] = owned

    for i in range(len(STEPS)):
        par_row(i).wait_send()
        over_chips(i).wait_send()
    for k in range(1, ZS):
        par_z(k).wait_send()
        over_z(k).wait_send()
    par_core().wait_send()
    over_core.wait_send()
    over_side.wait_send()

    @pl.loop(0, imgs)
    def _(j):
        all_of(go.at[j], go_s.at[j]).wait()
        all_of(low_s.at[j], low_ss.at[j]).wait()
        all_of(gc_s.at[j], gc_ss.at[j]).wait()
        all_of(send_a.at[pl.ds(0, 14)], as_sem.at[j]).wait()

    @pl.loop(0, 2 * imgs)
    def _(w):
        all_of(send_a.at[pl.ds(0, 7)], bs_sem.at[w]).wait()
        all_of(send_a.at[0], own_sem.at[2 * imgs + w]).wait()
        all_of(gso.at[pl.ds(0, 7)], br_sem.at[w]).wait()


def settle(gso, gt, gp, gso_out, gt_out, gp_out, perm, stage, sems):
    lanes, own = gso_out.shape[2], gso_out.shape[0]
    width = gso_out.shape[3]
    blocks = gso_out.shape[1]
    gt_copy = pltpu.make_async_copy(gt, gt_out, sems.at[0])
    gp_copy = pltpu.make_async_copy(gp, gp_out, sems.at[1])
    gt_copy.start()
    gp_copy.start()
    perm[...] = row_order(own, lanes, True)

    def put(g):
        return pltpu.make_async_copy(stage.at[g], gso_out.at[:, g], sems.at[2 + g])

    @pl.loop(0, blocks)
    def _(g):
        block = gso.at[pl.ds(g * lanes, lanes)].reshape(own * lanes, width)
        out = stage.at[g].reshape(own * lanes, width)
        for n in range(0, width, 256):
            out[:, n : n + 256] = dot(perm[...], block[:, n : n + 256], (((1,), (0,)), ((), ()))).astype(BF)
        put(g).start()

    @pl.loop(0, blocks)
    def _(g):
        put(g).wait()

    gt_copy.wait()
    gp_copy.wait()


def per_device(tokens, grad_out, slot_out, slot_params):
    toks, imgs, width = tokens.shape
    own, all_imgs, _ = slot_out.shape
    lanes = 8
    blocks = all_imgs // lanes
    slots = CHIPS * CORES * own
    tok = jnp.swapaxes(tokens, 0, 1)
    go = jnp.swapaxes(grad_out, 0, 1)
    so = slot_out.reshape(own, blocks, lanes, width)
    sp = slot_params.reshape(ZS, own // ZS, width)
    piece = width // (NEAR * ZS)
    anywhere = pl.BlockSpec(memory_space=pl.ANY)
    vmem = pl.BlockSpec(memory_space=pltpu.VMEM)
    dma = pltpu.SemaphoreType.DMA
    gso, gt, gp = pl.pallas_call(
        exchange,
        out_shape=(
            pltpu.VMEM((all_imgs, own, width), BF),
            pltpu.VMEM((imgs, toks, width), BF),
            pltpu.VMEM((own, piece), F32),
        ),
        in_specs=[anywhere] * 4,
        out_specs=(vmem, vmem, vmem),
        scratch_shapes=[
            pltpu.VMEM((imgs, toks, width), BF),
            pltpu.VMEM((2 * imgs, toks, width), BF),
            pltpu.VMEM((blocks, own, lanes, width), BF),
            pltpu.VMEM((all_imgs, own, width), BF),
            pltpu.VMEM((2 * imgs, 4, CORES, own, width), BF),
            pltpu.VMEM((2 * imgs, 4, CORES, own, width), BF),
            pltpu.VMEM((CHIPS, CORES, ZS, own // ZS, width), BF),
            pltpu.VMEM((imgs, CHIPS, CORES * own, toks), F32),
            pltpu.VMEM((2 * imgs, 4, CORES * own, toks), BF),
            pltpu.VMEM((imgs, 4, CORES * own, toks), BF),
            pltpu.VMEM((imgs, 4, CORES * own, toks), BF),
            pltpu.VMEM((imgs, 4, CORES * own, toks), BF),
            pltpu.VMEM((CHIPS, CORES * own, toks), F32),
            pltpu.VMEM((slots, width), F32),
            pltpu.VMEM((own * lanes, own * lanes), BF),
            pltpu.VMEM((CHIPS, own, width), BF),
            pltpu.VMEM((CHIPS, own, width), BF),
            pltpu.VMEM((ZS, NEAR, CHIPS * own, piece), F32),
            pltpu.VMEM((ZS, NEAR, CHIPS * own, piece), BF),
            pltpu.VMEM((ZS - 1, NEAR, CHIPS * own, piece), BF),
            pltpu.VMEM((CHIPS * own, piece), BF),
            pltpu.VMEM((CHIPS * own, piece), BF),
            pltpu.VMEM((CHIPS, own, piece), BF),
            pltpu.VMEM((CHIPS - 1, own, piece), BF),
            dma((blocks,)),
            dma((3,)),
            dma((CHIPS + ZS - 1,)),
            dma((CHIPS + ZS - 1,)),
            dma((imgs,)),
            dma((imgs,)),
            dma((imgs,)),
            dma((2 * imgs,)),
            dma((2 * imgs,)),
            dma((2 * imgs,)),
            dma((imgs,)),
            dma((imgs,)),
            dma((imgs,)),
            dma((imgs,)),
            dma((4 * imgs,)),
            dma((ZS + CHIPS,)),
            dma((ZS + CHIPS,)),
        ],
        compiler_params=pltpu.CompilerParams(
            collective_id=0, has_side_effects=True, vmem_limit_bytes=52 * 2**20
        ),
        name="exchange",
    )(tok, go, so, sp)
    gso_out, gt_out, gp_out = pl.pallas_call(
        settle,
        out_shape=(
            jax.ShapeDtypeStruct((own, blocks, lanes, width), BF),
            jax.ShapeDtypeStruct((imgs, toks, width), BF),
            jax.ShapeDtypeStruct((own, piece), F32),
        ),
        in_specs=[vmem] * 3,
        out_specs=(anywhere,) * 3,
        scratch_shapes=[
            pltpu.VMEM((own * lanes, own * lanes), BF),
            pltpu.VMEM((blocks, own, lanes, width), BF),
            dma((2 + blocks,)),
        ],
        compiler_params=pltpu.CompilerParams(vmem_limit_bytes=20 * 2**20),
        name="settle",
    )(gso, gt, gp)
    return (
        jnp.swapaxes(gt_out, 0, 1),
        gso_out.reshape(own, all_imgs, width),
        gp_out,
    )


def solution(mesh):
    return jax.shard_map(
        per_device,
        mesh=mesh,
        in_specs=(
            P(None, ("dp", "expert"), None),
            P(None, ("dp", "expert"), None),
            P("expert", "dp", None),
            P("expert", None),
        ),
        out_specs=(P(None, ("dp", "expert"), None), P("expert", "dp", None), P("expert", "dp")),
        check_vma=False,
    )
```

```python
import functools

import jax
import jax.numpy as jnp
from jax import lax
from jax.experimental import pallas as pl
from jax.experimental.pallas import tpu as pltpu
from jax.sharding import PartitionSpec as P

MESH = pl.DeviceIdType.MESH
BF = jnp.bfloat16
F32 = jnp.float32

ROWS, XS, CORES = 2, 4, 2
NEAR, ZS = 2, 4
CHIPS = ROWS * XS
STEPS = ((1, 0), (1, 2), (0, 1), (0, 3), (1, 1), (1, 3), (0, 2))
ORDER = tuple((r, x, c) for c in range(CORES) for r, x in STEPS) + ((0, 0, 1),)
NT = (((1,), (1,)), ((), ()))
TN = (((0,), (0,)), ((), ()))
NN = (((1,), (0,)), ((), ()))
KINDS = (0, 1, 2)
HELPER = ((1, 0), (0, 1), (0, 3))
PARTS = (
    (((0, 0), (0, 1), (0, 2), (0, 3)), ((0, 0), (1, 0), (0, 3), (1, 3)), ((0, 0), (1, 0), (0, 1), (1, 1))),
    (((0, 0), (0, 1), (0, 2), (0, 3)), ((0, 0), (1, 0), (0, 1), (1, 1)), ((0, 0), (1, 0), (0, 3), (1, 3))),
)
PIECES = 4
MIX = tuple(kind * 8 + k * CORES + dc for dc in range(CORES) for k in (3, 1, 2, 0) for kind in (0, 1))
BACK = tuple(tuple(tuple((k, of[k]) for k in (3, 1, 2, 0)) for of in kind) for kind in PARTS)


def back(at):
    return ((ROWS - at[0]) % ROWS, (XS - at[1]) % XS)


def add(a, b):
    return ((a[0] + b[0]) % ROWS, (a[1] + b[1]) % XS)


def dot(a, b, dims):
    return lax.dot_general(a, b, dims, preferred_element_type=F32)


def row_order(own, lanes, flip):
    n = own * lanes
    r = lax.broadcasted_iota(jnp.int32, (n, n), 0)
    c = lax.broadcasted_iota(jnp.int32, (n, n), 1)
    if flip:
        hit = c == (r % lanes) * own + r // lanes
    else:
        hit = c == (r % own) * lanes + r // own
    return jnp.where(hit, 1.0, 0.0).astype(BF)


def exchange(
    tok_hbm, go_hbm, so_hbm, sp_hbm,
    gso, gt, gp,
    tok, go, raw, send_a, slot_in, send_b, par, comb, low_w, low_s, gc_s, gc_r, gc_all, pp, perm,
    r1s, r1r, acc, r2s, r2r, r3s, r3r, r4s, r4r,
    so_sem, in_sem, par_s, par_r, go_s, go_r, as_sem, ar_sem, bs_sem, br_sem,
    low_ss, low_rs, gc_ss, gc_rs, own_sem, red_s, red_r,
):
    imgs, width, tokens = tok.shape[0], tok.shape[2], tok.shape[1]
    blocks, own, lanes = raw.shape[0], so_hbm.shape[0], so_hbm.shape[2]
    slots = CHIPS * CORES * own
    half = slots // 2
    rounds = imgs // len(KINDS)
    d = lax.axis_index("dp")
    e = lax.axis_index("expert")
    row, x, c = e // (XS * CORES), (e // CORES) % XS, e % CORES
    chip = e // CORES
    near, z = d // ZS, d % ZS

    def chip_at(dr, dx):
        return ((row + dr) % ROWS) * XS + (x + dx) % XS

    def peer(dr, dx, dc):
        return chip_at(dr, dx) * CORES + (c + dc) % CORES

    def zpeer(k):
        return (near * ZS + (z + k) % ZS, e)

    side = ((1 - near) * ZS + z, e)
    partner = (d, peer(0, 0, 1))

    barrier = pltpu.get_barrier_semaphore()
    others = [(d, peer(*o)) for o in ORDER] + [zpeer(k) for k in range(1, ZS)] + [side]
    for dev in others:
        pl.semaphore_signal(barrier, inc=1, device_id=dev, device_id_type=MESH)

    def load_so(g):
        return pltpu.make_async_copy(so_hbm.at[:, g], raw.at[g], so_sem.at[g])

    sp_in = pltpu.make_async_copy(sp_hbm.at[z], par.at[chip, c, z], in_sem.at[0])
    go_in = pltpu.make_async_copy(go_hbm, go.at[pl.ds(0, imgs)], in_sem.at[1])
    tok_in = pltpu.make_async_copy(tok_hbm, tok, in_sem.at[2])
    sp_in.start()
    go_in.start()
    for g in range(blocks):
        load_so(g).start()
    tok_in.start()
    perm[...] = row_order(own, lanes, False)

    pl.semaphore_wait(barrier, len(others))

    def remote(src, dst, s, r, dev):
        return pltpu.make_async_remote_copy(
            src_ref=src, dst_ref=dst, send_sem=s, recv_sem=r, device_id=dev, device_id_type=MESH
        )

    def all_of(ref, sem):
        return pltpu.make_async_copy(ref, ref, sem)

    def par_row(i):
        r, dx = STEPS[i]
        piece = par.at[chip, c, z]
        return remote(piece, piece, par_s.at[i], par_r.at[i], (d, peer(r, dx, 0)))

    def par_z(k):
        piece = par.at[:, c, z]
        n = len(STEPS) + k - 1
        return remote(piece, piece, par_s.at[n], par_r.at[n], zpeer(k))

    def par_core():
        piece = par.at[:, c]
        n = len(STEPS) + ZS - 1
        return remote(piece, piece, par_s.at[n], par_r.at[n], partner)

    sp_in.wait()
    for i in range(len(STEPS)):
        par_row(i).start()

    def helper(t):
        return (d, peer(*HELPER[t], 0))

    def home(t):
        return (d, peer(*back(HELPER[t]), 0))

    go_in.wait()
    step = tokens // PIECES
    for q in range(PIECES):
        for j in range(imgs):
            rows = pl.ds(q * step, step)
            remote(
                go.at[j, rows], go.at[imgs + j, rows], go_s.at[j], go_r.at[j], helper(j % len(KINDS))
            ).start()

    @pl.loop(0, blocks)
    def _(g):
        load_so(g).wait()
        block = raw.at[g].reshape(own * lanes, width)
        out = send_a.at[pl.ds(g * lanes, lanes)].reshape(own * lanes, width)
        for n in range(0, width, 256):
            out[:, n : n + 256] = dot(perm[...], block[:, n : n + 256], NN).astype(BF)

    def out_moves(j, t):
        for kind in range(2):
            for k, (dr, dx) in enumerate(PARTS[kind][t]):
                for dc in range(CORES):
                    at = back((dr, dx))
                    hr, hx = at if kind == 0 else add(at, back(HELPER[t]))
                    image = peer(hr, hx, dc) * imgs + j
                    yield kind, k, (*at, dc), send_a.at[image], slot_in.at[kind * imgs + j, k, c]

    def send_out(j, t, kinds):
        moves = list(out_moves(j, t))
        for i in MIX:
            kind, _, o, src, dst = moves[i]
            if kind not in kinds:
                continue
            w = kind * imgs + j
            if o == (0, 0, 0):
                pltpu.make_async_copy(src, dst, own_sem.at[w]).start()
            else:
                remote(src, dst, as_sem.at[j], ar_sem.at[w], (d, peer(*o))).start()

    def wait_out(w):
        all_of(slot_in.at[w].reshape(2 * len(PARTS[0][0]), own, width).at[pl.ds(0, 7)], ar_sem.at[w]).wait()
        all_of(send_a.at[0], own_sem.at[w]).wait()

    def send_back(kind, j, t):
        hr, hx = (0, 0) if kind == 0 else back(HELPER[t])
        image = peer(hr, hx, 0) * imgs + j
        w = kind * imgs + j
        for dc in range(CORES):
            for k, (dr, dx) in BACK[kind][t]:
                src, dst = send_b.at[w, k, (c + dc) % CORES], gso.at[image]
                if (dr, dx, dc) == (0, 0, 0):
                    pltpu.make_async_copy(src, dst, own_sem.at[2 * imgs + w]).start()
                else:
                    remote(src, dst, bs_sem.at[w], br_sem.at[w], (d, peer(dr, dx, dc))).start()

    for t in range(len(KINDS)):
        send_out(t, t, (0, 1))

    for i in range(len(STEPS)):
        par_row(i).wait_recv()
    for k in range(1, ZS):
        par_z(k).start()
    for k in range(1, ZS):
        par_z(k).wait_recv()
    par_core().start()
    par_core().wait_recv()
    tok_in.wait()

    params = par.reshape(slots, width)

    def part_chips(kind, t):
        at = (0, 0) if kind == 0 else HELPER[t]
        return [chip_at(*add(at, p)) for p in PARTS[kind][t]]

    def send_low(j, t):
        return remote(low_s.at[j], low_w.at[imgs + j], low_ss.at[j], low_rs.at[j], helper(t))

    @pl.loop(0, rounds)
    def _(r):
        for t in range(len(KINDS)):
            j = r * len(KINDS) + t
            logits = dot(params[...], tok[j], NT)
            top = jnp.max(logits, axis=0, keepdims=True)
            raised = jnp.exp(logits - top)
            weight = raised / jnp.sum(raised, axis=0, keepdims=True)
            comb[j] = weight.reshape(CHIPS, CORES * own, tokens)
            for k, p in enumerate(part_chips(0, t)):
                low_w[j, k] = comb[j, p].astype(BF)
            for k, p in enumerate(part_chips(1, t)):
                low_s[j, k] = comb[j, p].astype(BF)
            if t > 0:
                send_low(j - 1, t - 1).start()
        send_low(r * len(KINDS) + len(KINDS) - 1, len(KINDS) - 1).start()

    for kind in (1, 0):
        for t in range(len(KINDS)):
            send_out(len(KINDS) + t, t, (kind,))

    def slot_grads(w):
        low = low_w[w].reshape(half, tokens)
        out = send_b.at[w].reshape(half, width)
        for n in range(0, width, 256):
            out[:, n : n + 256] = dot(low, go[w, :, n : n + 256], NN).astype(BF)

    @pl.loop(0, imgs)
    def _(j):
        slot_grads(j)

    def logit_dot(w):
        return dot(slot_in[w].reshape(half, width), go[w], NT).reshape(-1, CORES * own, tokens)

    def send_gc(j, t):
        return remote(gc_s.at[j], gc_r.at[j], gc_ss.at[j], gc_rs.at[j], home(t))

    @pl.loop(0, rounds)
    def _(r):
        for t in range(len(KINDS)):
            j = r * len(KINDS) + t
            all_of(low_w.at[imgs + j], low_rs.at[j]).wait()
            all_of(go.at[imgs + j], go_r.at[j]).wait()
            slot_grads(imgs + j)
            wait_out(imgs + j)
            gc_s[j] = logit_dot(imgs + j).astype(BF)
            if t > 0:
                send_gc(j - 1, t - 1).start()
        send_gc(r * len(KINDS) + len(KINDS) - 1, len(KINDS) - 1).start()

    for j in range(imgs):
        send_back(0, j, j % len(KINDS))
    pp[...] = jnp.zeros_like(pp)

    @pl.loop(0, rounds)
    def _(r):
        for t in range(len(KINDS)):
            j = r * len(KINDS) + t
            wait_out(j)
            part = logit_dot(j)
            for k, p in enumerate(part_chips(0, t)):
                gc_all[p] = part[k]
            send_gc(j, t).wait_recv()
            for k, p in enumerate(part_chips(1, t)):
                gc_all[p] = gc_r[j, k].astype(F32)
            grad = gc_all[...].reshape(slots, tokens)
            weight = comb[j].reshape(slots, tokens)
            rowdot = jnp.sum(weight * grad, axis=0, keepdims=True)
            low = (weight * (grad - rowdot)).astype(BF)
            for n in range(0, width, 256):
                pp[:, n : n + 256] += dot(low, tok[j, :, n : n + 256], NN)
                gt[j, :, n : n + 256] = dot(low, params[:, n : n + 256], TN).astype(BF)

    share = pp.reshape(CHIPS, CORES, own, width)
    r1s[...] = share[:, 1 - c].astype(BF)
    over_core = remote(r1s, r1r, red_s.at[0], red_r.at[0], partner)
    for t in (0, 1):
        send_back(1, t, t)
    over_core.start()
    over_core.wait_recv()
    both = (share[:, c] + r1r[...].astype(F32)).reshape(CHIPS * own, width)
    piece = width // (NEAR * ZS)
    for n in range(NEAR):
        for k in range(ZS):
            m = (n * ZS + k) * piece
            acc[k, n] = both[:, m : m + piece]
    r2s[...] = acc[...].astype(BF)

    def over_z(k):
        return remote(r2s.at[(z + k) % ZS], r2r.at[k - 1], red_s.at[k], red_r.at[k], zpeer(k))

    for k in range(1, ZS):
        over_z(k).start()
    total = acc[z]
    for k in range(1, ZS):
        over_z(k).wait_recv()
        total = total + r2r[k - 1].astype(F32)
    acc[0] = total
    r3s[...] = acc[0, 1 - near].astype(BF)
    over_side = remote(r3s, r3r, red_s.at[ZS], red_r.at[ZS], side)
    over_side.start()
    send_back(1, 2, 2)
    send_back(1, len(KINDS), 0)
    over_side.wait_recv()
    mine = (acc[0, near] + r3r[...].astype(F32)).reshape(CHIPS, own, piece)
    r4s[...] = mine.astype(BF)
    acc[1, 0] = mine.reshape(CHIPS * own, piece)

    def over_chips(i):
        p = peer(*STEPS[i], 0)
        return remote(r4s.at[p // CORES], r4r.at[i], red_s.at[ZS + 1 + i], red_r.at[ZS + 1 + i], (d, p))

    for i in range(len(STEPS)):
        over_chips(i).start()
    for t in (1, 2):
        send_back(1, len(KINDS) + t, t)
    owned = acc.at[1, 0].reshape(CHIPS, own, piece)[chip]
    for i in range(len(STEPS)):
        over_chips(i).wait_recv()
        owned = owned + r4r[i].astype(F32)
    gp[...] = owned

    for i in range(len(STEPS)):
        par_row(i).wait_send()
        over_chips(i).wait_send()
    for k in range(1, ZS):
        par_z(k).wait_send()
        over_z(k).wait_send()
    par_core().wait_send()
    over_core.wait_send()
    over_side.wait_send()

    @pl.loop(0, imgs)
    def _(j):
        all_of(go.at[j], go_s.at[j]).wait()
        all_of(low_s.at[j], low_ss.at[j]).wait()
        all_of(gc_s.at[j], gc_ss.at[j]).wait()
        all_of(send_a.at[pl.ds(0, 14)], as_sem.at[j]).wait()

    @pl.loop(0, 2 * imgs)
    def _(w):
        all_of(send_a.at[pl.ds(0, 7)], bs_sem.at[w]).wait()
        all_of(send_a.at[0], own_sem.at[2 * imgs + w]).wait()
        all_of(gso.at[pl.ds(0, 7)], br_sem.at[w]).wait()


def settle(gso, gt, gp, gso_out, gt_out, gp_out, perm, stage, sems):
    lanes, own = gso_out.shape[2], gso_out.shape[0]
    width = gso_out.shape[3]
    blocks = gso_out.shape[1]
    gt_copy = pltpu.make_async_copy(gt, gt_out, sems.at[0])
    gp_copy = pltpu.make_async_copy(gp, gp_out, sems.at[1])
    gt_copy.start()
    gp_copy.start()
    perm[...] = row_order(own, lanes, True)

    def put(g):
        return pltpu.make_async_copy(stage.at[g], gso_out.at[:, g], sems.at[2 + g])

    @pl.loop(0, blocks // 4)
    def _(h):
        for g in range(4):
            block = gso.at[pl.ds((h * 4 + g) * lanes, lanes)].reshape(own * lanes, width)
            out = stage.at[h * 4 + g].reshape(own * lanes, width)
            out[...] = dot(perm[...], block[...], NN).astype(BF)
        for g in range(4):
            put(h * 4 + g).start()

    @pl.loop(0, blocks)
    def _(g):
        put(g).wait()

    gt_copy.wait()
    gp_copy.wait()


def per_device(tokens, grad_out, slot_out, slot_params):
    toks, imgs, width = tokens.shape
    own, all_imgs, _ = slot_out.shape
    lanes = 8
    blocks = all_imgs // lanes
    slots = CHIPS * CORES * own
    tok = jnp.swapaxes(tokens, 0, 1)
    go = jnp.swapaxes(grad_out, 0, 1)
    so = slot_out.reshape(own, blocks, lanes, width)
    sp = slot_params.reshape(ZS, own // ZS, width)
    piece = width // (NEAR * ZS)
    anywhere = pl.BlockSpec(memory_space=pl.ANY)
    vmem = pl.BlockSpec(memory_space=pltpu.VMEM)
    dma = pltpu.SemaphoreType.DMA
    gso, gt, gp = pl.pallas_call(
        exchange,
        out_shape=(
            pltpu.VMEM((all_imgs, own, width), BF),
            pltpu.VMEM((imgs, toks, width), BF),
            pltpu.VMEM((own, piece), F32),
        ),
        in_specs=[anywhere] * 4,
        out_specs=(vmem, vmem, vmem),
        scratch_shapes=[
            pltpu.VMEM((imgs, toks, width), BF),
            pltpu.VMEM((2 * imgs, toks, width), BF),
            pltpu.VMEM((blocks, own, lanes, width), BF),
            pltpu.VMEM((all_imgs, own, width), BF),
            pltpu.VMEM((2 * imgs, 4, CORES, own, width), BF),
            pltpu.VMEM((2 * imgs, 4, CORES, own, width), BF),
            pltpu.VMEM((CHIPS, CORES, ZS, own // ZS, width), BF),
            pltpu.VMEM((imgs, CHIPS, CORES * own, toks), F32),
            pltpu.VMEM((2 * imgs, 4, CORES * own, toks), BF),
            pltpu.VMEM((imgs, 4, CORES * own, toks), BF),
            pltpu.VMEM((imgs, 4, CORES * own, toks), BF),
            pltpu.VMEM((imgs, 4, CORES * own, toks), BF),
            pltpu.VMEM((CHIPS, CORES * own, toks), F32),
            pltpu.VMEM((slots, width), F32),
            pltpu.VMEM((own * lanes, own * lanes), BF),
            pltpu.VMEM((CHIPS, own, width), BF),
            pltpu.VMEM((CHIPS, own, width), BF),
            pltpu.VMEM((ZS, NEAR, CHIPS * own, piece), F32),
            pltpu.VMEM((ZS, NEAR, CHIPS * own, piece), BF),
            pltpu.VMEM((ZS - 1, NEAR, CHIPS * own, piece), BF),
            pltpu.VMEM((CHIPS * own, piece), BF),
            pltpu.VMEM((CHIPS * own, piece), BF),
            pltpu.VMEM((CHIPS, own, piece), BF),
            pltpu.VMEM((CHIPS - 1, own, piece), BF),
            dma((blocks,)),
            dma((3,)),
            dma((CHIPS + ZS - 1,)),
            dma((CHIPS + ZS - 1,)),
            dma((imgs,)),
            dma((imgs,)),
            dma((imgs,)),
            dma((2 * imgs,)),
            dma((2 * imgs,)),
            dma((2 * imgs,)),
            dma((imgs,)),
            dma((imgs,)),
            dma((imgs,)),
            dma((imgs,)),
            dma((4 * imgs,)),
            dma((ZS + CHIPS,)),
            dma((ZS + CHIPS,)),
        ],
        compiler_params=pltpu.CompilerParams(
            collective_id=0, has_side_effects=True, vmem_limit_bytes=52 * 2**20
        ),
        name="exchange",
    )(tok, go, so, sp)
    gso_out, gt_out, gp_out = pl.pallas_call(
        settle,
        out_shape=(
            jax.ShapeDtypeStruct((own, blocks, lanes, width), BF),
            jax.ShapeDtypeStruct((imgs, toks, width), BF),
            jax.ShapeDtypeStruct((own, piece), F32),
        ),
        in_specs=[vmem] * 3,
        out_specs=(anywhere,) * 3,
        scratch_shapes=[
            pltpu.VMEM((own * lanes, own * lanes), BF),
            pltpu.VMEM((blocks, own, lanes, width), BF),
            dma((2 + blocks,)),
        ],
        compiler_params=pltpu.CompilerParams(vmem_limit_bytes=20 * 2**20),
        name="settle",
    )(gso, gt, gp)
    return (
        jnp.swapaxes(gt_out, 0, 1),
        gso_out.reshape(own, all_imgs, width),
        gp_out,
    )


def solution(mesh):
    return jax.shard_map(
        per_device,
        mesh=mesh,
        in_specs=(
            P(None, ("dp", "expert"), None),
            P(None, ("dp", "expert"), None),
            P("expert", "dp", None),
            P("expert", None),
        ),
        out_specs=(P(None, ("dp", "expert"), None), P("expert", "dp", None), P("expert", "dp")),
        check_vma=False,
    )
```

```python
import functools

import jax
import jax.numpy as jnp
from jax import lax
from jax.experimental import pallas as pl
from jax.experimental.pallas import tpu as pltpu
from jax.sharding import PartitionSpec as P

MESH = pl.DeviceIdType.MESH
BF = jnp.bfloat16
F32 = jnp.float32

ROWS, XS, CORES = 2, 4, 2
NEAR, ZS = 2, 4
CHIPS = ROWS * XS
STEPS = ((1, 0), (1, 2), (0, 1), (0, 3), (1, 1), (1, 3), (0, 2))
ORDER = tuple((r, x, c) for c in range(CORES) for r, x in STEPS) + ((0, 0, 1),)
NT = (((1,), (1,)), ((), ()))
TN = (((0,), (0,)), ((), ()))
NN = (((1,), (0,)), ((), ()))
KINDS = (0, 1, 2)
HELPER = ((1, 0), (0, 1), (0, 3))
PARTS = (
    (((0, 0), (0, 1), (0, 2), (0, 3)), ((0, 0), (1, 0), (0, 3), (1, 3)), ((0, 0), (1, 0), (0, 1), (1, 1))),
    (((0, 0), (0, 1), (0, 2), (0, 3)), ((0, 0), (1, 0), (0, 1), (1, 1)), ((0, 0), (1, 0), (0, 3), (1, 3))),
)
PIECES = 4
MIX = tuple(kind * 8 + k * CORES + dc for dc in range(CORES) for k in (3, 1, 2, 0) for kind in (0, 1))
BACK = tuple(tuple(tuple((k, of[k]) for k in (3, 1, 2, 0)) for of in kind) for kind in PARTS)


def back(at):
    return ((ROWS - at[0]) % ROWS, (XS - at[1]) % XS)


def add(a, b):
    return ((a[0] + b[0]) % ROWS, (a[1] + b[1]) % XS)


def dot(a, b, dims):
    return lax.dot_general(a, b, dims, preferred_element_type=F32)


def row_order(own, lanes, flip):
    n = own * lanes
    r = lax.broadcasted_iota(jnp.int32, (n, n), 0)
    c = lax.broadcasted_iota(jnp.int32, (n, n), 1)
    if flip:
        hit = c == (r % lanes) * own + r // lanes
    else:
        hit = c == (r % own) * lanes + r // own
    return jnp.where(hit, 1.0, 0.0).astype(BF)


def exchange(
    tok_hbm, go_hbm, so_hbm, sp_hbm,
    gso, gt, gp,
    tok, go, raw, send_a, slot_in, send_b, par, comb, low_w, low_s, gc_s, gc_r, gc_all, pp, perm,
    r1s, r1r, acc, r2s, r2r, r3s, r3r, r4s, r4r,
    so_sem, in_sem, par_s, par_r, go_s, go_r, as_sem, ar_sem, bs_sem, br_sem,
    low_ss, low_rs, gc_ss, gc_rs, own_sem, red_s, red_r,
):
    imgs, width, tokens = tok.shape[0], tok.shape[2], tok.shape[1]
    blocks, own, lanes = raw.shape[0], so_hbm.shape[0], so_hbm.shape[2]
    slots = CHIPS * CORES * own
    half = slots // 2
    rounds = imgs // len(KINDS)
    d = lax.axis_index("dp")
    e = lax.axis_index("expert")
    row, x, c = e // (XS * CORES), (e // CORES) % XS, e % CORES
    chip = e // CORES
    near, z = d // ZS, d % ZS

    def chip_at(dr, dx):
        return ((row + dr) % ROWS) * XS + (x + dx) % XS

    def peer(dr, dx, dc):
        return chip_at(dr, dx) * CORES + (c + dc) % CORES

    def zpeer(k):
        return (near * ZS + (z + k) % ZS, e)

    side = ((1 - near) * ZS + z, e)
    partner = (d, peer(0, 0, 1))

    barrier = pltpu.get_barrier_semaphore()
    others = [(d, peer(*o)) for o in ORDER] + [zpeer(k) for k in range(1, ZS)] + [side]
    for dev in others:
        pl.semaphore_signal(barrier, inc=1, device_id=dev, device_id_type=MESH)

    def load_so(g):
        return pltpu.make_async_copy(so_hbm.at[:, g], raw.at[g], so_sem.at[g])

    sp_in = pltpu.make_async_copy(sp_hbm.at[z], par.at[chip, c, z], in_sem.at[0])
    go_in = pltpu.make_async_copy(go_hbm, go.at[pl.ds(0, imgs)], in_sem.at[1])
    tok_in = pltpu.make_async_copy(tok_hbm, tok, in_sem.at[2])
    sp_in.start()
    go_in.start()
    for g in range(blocks):
        load_so(g).start()
    tok_in.start()
    perm[...] = row_order(own, lanes, False)

    pl.semaphore_wait(barrier, len(others))

    def remote(src, dst, s, r, dev):
        return pltpu.make_async_remote_copy(
            src_ref=src, dst_ref=dst, send_sem=s, recv_sem=r, device_id=dev, device_id_type=MESH
        )

    def all_of(ref, sem):
        return pltpu.make_async_copy(ref, ref, sem)

    def par_row(i):
        r, dx = STEPS[i]
        piece = par.at[chip, c, z]
        return remote(piece, piece, par_s.at[i], par_r.at[i], (d, peer(r, dx, 0)))

    def par_z(k):
        piece = par.at[:, c, z]
        n = len(STEPS) + k - 1
        return remote(piece, piece, par_s.at[n], par_r.at[n], zpeer(k))

    def par_core():
        piece = par.at[:, c]
        n = len(STEPS) + ZS - 1
        return remote(piece, piece, par_s.at[n], par_r.at[n], partner)

    sp_in.wait()
    for i in range(len(STEPS)):
        par_row(i).start()

    def helper(t):
        return (d, peer(*HELPER[t], 0))

    def home(t):
        return (d, peer(*back(HELPER[t]), 0))

    go_in.wait()
    step = tokens // PIECES
    for q in range(PIECES):
        for j in range(imgs):
            rows = pl.ds(q * step, step)
            remote(
                go.at[j, rows], go.at[imgs + j, rows], go_s.at[j], go_r.at[j], helper(j % len(KINDS))
            ).start()

    @pl.loop(0, blocks)
    def _(g):
        load_so(g).wait()
        block = raw.at[g].reshape(own * lanes, width)
        out = send_a.at[pl.ds(g * lanes, lanes)].reshape(own * lanes, width)
        for n in range(0, width, 256):
            out[:, n : n + 256] = dot(perm[...], block[:, n : n + 256], NN).astype(BF)

    def out_moves(j, t):
        for kind in range(2):
            for k, (dr, dx) in enumerate(PARTS[kind][t]):
                for dc in range(CORES):
                    at = back((dr, dx))
                    hr, hx = at if kind == 0 else add(at, back(HELPER[t]))
                    image = peer(hr, hx, dc) * imgs + j
                    yield kind, k, (*at, dc), send_a.at[image], slot_in.at[kind * imgs + j, k, c]

    def send_out(j, t, kinds):
        moves = list(out_moves(j, t))
        for i in MIX:
            kind, _, o, src, dst = moves[i]
            if kind not in kinds:
                continue
            w = kind * imgs + j
            if o == (0, 0, 0):
                pltpu.make_async_copy(src, dst, own_sem.at[w]).start()
            else:
                remote(src, dst, as_sem.at[j], ar_sem.at[w], (d, peer(*o))).start()

    def wait_out(w):
        all_of(slot_in.at[w].reshape(2 * len(PARTS[0][0]), own, width).at[pl.ds(0, 7)], ar_sem.at[w]).wait()
        all_of(send_a.at[0], own_sem.at[w]).wait()

    def send_back(kind, r, dcs):
        for dc in dcs:
            for i in range(4):
                for t in range(len(KINDS)):
                    j = r * len(KINDS) + t
                    hr, hx = (0, 0) if kind == 0 else back(HELPER[t])
                    w = kind * imgs + j
                    k, (dr, dx) = BACK[kind][t][i]
                    src, dst = send_b.at[w, k, (c + dc) % CORES], gso.at[peer(hr, hx, 0) * imgs + j]
                    if (dr, dx, dc) == (0, 0, 0):
                        pltpu.make_async_copy(src, dst, own_sem.at[2 * imgs + w]).start()
                    else:
                        remote(src, dst, bs_sem.at[w], br_sem.at[w], (d, peer(dr, dx, dc))).start()

    for t in range(len(KINDS)):
        send_out(t, t, (0, 1))

    for i in range(len(STEPS)):
        par_row(i).wait_recv()
    for k in range(1, ZS):
        par_z(k).start()
    for k in range(1, ZS):
        par_z(k).wait_recv()
    par_core().start()
    par_core().wait_recv()
    tok_in.wait()

    params = par.reshape(slots, width)

    def part_chips(kind, t):
        at = (0, 0) if kind == 0 else HELPER[t]
        return [chip_at(*add(at, p)) for p in PARTS[kind][t]]

    def send_low(j, t):
        return remote(low_s.at[j], low_w.at[imgs + j], low_ss.at[j], low_rs.at[j], helper(t))

    @pl.loop(0, rounds)
    def _(r):
        for t in range(len(KINDS)):
            j = r * len(KINDS) + t
            logits = dot(params[...], tok[j], NT)
            top = jnp.max(logits, axis=0, keepdims=True)
            raised = jnp.exp(logits - top)
            weight = raised / jnp.sum(raised, axis=0, keepdims=True)
            comb[j] = weight.reshape(CHIPS, CORES * own, tokens)
            for k, p in enumerate(part_chips(0, t)):
                low_w[j, k] = comb[j, p].astype(BF)
            for k, p in enumerate(part_chips(1, t)):
                low_s[j, k] = comb[j, p].astype(BF)
            if t > 0:
                send_low(j - 1, t - 1).start()
        send_low(r * len(KINDS) + len(KINDS) - 1, len(KINDS) - 1).start()

    for kind in (1, 0):
        for t in range(len(KINDS)):
            send_out(len(KINDS) + t, t, (kind,))

    def slot_grads(w):
        low = low_w[w].reshape(half, tokens)
        out = send_b.at[w].reshape(half, width)
        for n in range(0, width, 256):
            out[:, n : n + 256] = dot(low, go[w, :, n : n + 256], NN).astype(BF)

    @pl.loop(0, imgs)
    def _(j):
        slot_grads(j)

    def logit_dot(w):
        return dot(slot_in[w].reshape(half, width), go[w], NT).reshape(-1, CORES * own, tokens)

    def send_gc(j, t):
        return remote(gc_s.at[j], gc_r.at[j], gc_ss.at[j], gc_rs.at[j], home(t))

    @pl.loop(0, rounds)
    def _(r):
        for t in range(len(KINDS)):
            j = r * len(KINDS) + t
            all_of(low_w.at[imgs + j], low_rs.at[j]).wait()
            all_of(go.at[imgs + j], go_r.at[j]).wait()
            slot_grads(imgs + j)
            wait_out(imgs + j)
            gc_s[j] = logit_dot(imgs + j).astype(BF)
            if t > 0:
                send_gc(j - 1, t - 1).start()
        send_gc(r * len(KINDS) + len(KINDS) - 1, len(KINDS) - 1).start()

    for r in range(rounds):
        send_back(0, r, (0, 1))
    pp[...] = jnp.zeros_like(pp)

    @pl.loop(0, rounds)
    def _(r):
        for t in range(len(KINDS)):
            j = r * len(KINDS) + t
            wait_out(j)
            part = logit_dot(j)
            for k, p in enumerate(part_chips(0, t)):
                gc_all[p] = part[k]
            send_gc(j, t).wait_recv()
            for k, p in enumerate(part_chips(1, t)):
                gc_all[p] = gc_r[j, k].astype(F32)
            grad = gc_all[...].reshape(slots, tokens)
            weight = comb[j].reshape(slots, tokens)
            rowdot = jnp.sum(weight * grad, axis=0, keepdims=True)
            low = (weight * (grad - rowdot)).astype(BF)
            for n in range(0, width, 256):
                pp[:, n : n + 256] += dot(low, tok[j, :, n : n + 256], NN)
                gt[j, :, n : n + 256] = dot(low, params[:, n : n + 256], TN).astype(BF)

    share = pp.reshape(CHIPS, CORES, own, width)
    r1s[...] = share[:, 1 - c].astype(BF)
    over_core = remote(r1s, r1r, red_s.at[0], red_r.at[0], partner)
    send_back(1, 0, (0, 1))
    over_core.start()
    over_core.wait_recv()
    both = (share[:, c] + r1r[...].astype(F32)).reshape(CHIPS * own, width)
    piece = width // (NEAR * ZS)
    for n in range(NEAR):
        for k in range(ZS):
            m = (n * ZS + k) * piece
            acc[k, n] = both[:, m : m + piece]
    r2s[...] = acc[...].astype(BF)

    def over_z(k):
        return remote(r2s.at[(z + k) % ZS], r2r.at[k - 1], red_s.at[k], red_r.at[k], zpeer(k))

    for k in range(1, ZS):
        over_z(k).start()
    total = acc[z]
    for k in range(1, ZS):
        over_z(k).wait_recv()
        total = total + r2r[k - 1].astype(F32)
    acc[0] = total
    r3s[...] = acc[0, 1 - near].astype(BF)
    over_side = remote(r3s, r3r, red_s.at[ZS], red_r.at[ZS], side)
    over_side.start()
    send_back(1, 1, (0,))
    over_side.wait_recv()
    mine = (acc[0, near] + r3r[...].astype(F32)).reshape(CHIPS, own, piece)
    r4s[...] = mine.astype(BF)
    acc[1, 0] = mine.reshape(CHIPS * own, piece)

    def over_chips(i):
        p = peer(*STEPS[i], 0)
        return remote(r4s.at[p // CORES], r4r.at[i], red_s.at[ZS + 1 + i], red_r.at[ZS + 1 + i], (d, p))

    for i in range(len(STEPS)):
        over_chips(i).start()
    send_back(1, 1, (1,))
    owned = acc.at[1, 0].reshape(CHIPS, own, piece)[chip]
    for i in range(len(STEPS)):
        over_chips(i).wait_recv()
        owned = owned + r4r[i].astype(F32)
    gp[...] = owned

    for i in range(len(STEPS)):
        par_row(i).wait_send()
        over_chips(i).wait_send()
    for k in range(1, ZS):
        par_z(k).wait_send()
        over_z(k).wait_send()
    par_core().wait_send()
    over_core.wait_send()
    over_side.wait_send()

    @pl.loop(0, imgs)
    def _(j):
        all_of(go.at[j], go_s.at[j]).wait()
        all_of(low_s.at[j], low_ss.at[j]).wait()
        all_of(gc_s.at[j], gc_ss.at[j]).wait()
        all_of(send_a.at[pl.ds(0, 14)], as_sem.at[j]).wait()

    @pl.loop(0, 2 * imgs)
    def _(w):
        all_of(send_a.at[pl.ds(0, 7)], bs_sem.at[w]).wait()
        all_of(send_a.at[0], own_sem.at[2 * imgs + w]).wait()
        all_of(gso.at[pl.ds(0, 7)], br_sem.at[w]).wait()


def settle(gso, gt, gp, gso_out, gt_out, gp_out, perm, stage, sems):
    lanes, own = gso_out.shape[2], gso_out.shape[0]
    width = gso_out.shape[3]
    blocks = gso_out.shape[1]
    gt_copy = pltpu.make_async_copy(gt, gt_out, sems.at[0])
    gp_copy = pltpu.make_async_copy(gp, gp_out, sems.at[1])
    gt_copy.start()
    gp_copy.start()
    perm[...] = row_order(own, lanes, True)

    def put(g):
        return pltpu.make_async_copy(stage.at[g], gso_out.at[:, g], sems.at[2 + g])

    @pl.loop(0, blocks // 4)
    def _(h):
        for g in range(4):
            block = gso.at[pl.ds((h * 4 + g) * lanes, lanes)].reshape(own * lanes, width)
            out = stage.at[h * 4 + g].reshape(own * lanes, width)
            out[...] = dot(perm[...], block[...], NN).astype(BF)
        for g in range(4):
            put(h * 4 + g).start()

    @pl.loop(0, blocks)
    def _(g):
        put(g).wait()

    gt_copy.wait()
    gp_copy.wait()


def per_device(tokens, grad_out, slot_out, slot_params):
    toks, imgs, width = tokens.shape
    own, all_imgs, _ = slot_out.shape
    lanes = 8
    blocks = all_imgs // lanes
    slots = CHIPS * CORES * own
    tok = jnp.swapaxes(tokens, 0, 1)
    go = jnp.swapaxes(grad_out, 0, 1)
    so = slot_out.reshape(own, blocks, lanes, width)
    sp = slot_params.reshape(ZS, own // ZS, width)
    piece = width // (NEAR * ZS)
    anywhere = pl.BlockSpec(memory_space=pl.ANY)
    vmem = pl.BlockSpec(memory_space=pltpu.VMEM)
    dma = pltpu.SemaphoreType.DMA
    gso, gt, gp = pl.pallas_call(
        exchange,
        out_shape=(
            pltpu.VMEM((all_imgs, own, width), BF),
            pltpu.VMEM((imgs, toks, width), BF),
            pltpu.VMEM((own, piece), F32),
        ),
        in_specs=[anywhere] * 4,
        out_specs=(vmem, vmem, vmem),
        scratch_shapes=[
            pltpu.VMEM((imgs, toks, width), BF),
            pltpu.VMEM((2 * imgs, toks, width), BF),
            pltpu.VMEM((blocks, own, lanes, width), BF),
            pltpu.VMEM((all_imgs, own, width), BF),
            pltpu.VMEM((2 * imgs, 4, CORES, own, width), BF),
            pltpu.VMEM((2 * imgs, 4, CORES, own, width), BF),
            pltpu.VMEM((CHIPS, CORES, ZS, own // ZS, width), BF),
            pltpu.VMEM((imgs, CHIPS, CORES * own, toks), F32),
            pltpu.VMEM((2 * imgs, 4, CORES * own, toks), BF),
            pltpu.VMEM((imgs, 4, CORES * own, toks), BF),
            pltpu.VMEM((imgs, 4, CORES * own, toks), BF),
            pltpu.VMEM((imgs, 4, CORES * own, toks), BF),
            pltpu.VMEM((CHIPS, CORES * own, toks), F32),
            pltpu.VMEM((slots, width), F32),
            pltpu.VMEM((own * lanes, own * lanes), BF),
            pltpu.VMEM((CHIPS, own, width), BF),
            pltpu.VMEM((CHIPS, own, width), BF),
            pltpu.VMEM((ZS, NEAR, CHIPS * own, piece), F32),
            pltpu.VMEM((ZS, NEAR, CHIPS * own, piece), BF),
            pltpu.VMEM((ZS - 1, NEAR, CHIPS * own, piece), BF),
            pltpu.VMEM((CHIPS * own, piece), BF),
            pltpu.VMEM((CHIPS * own, piece), BF),
            pltpu.VMEM((CHIPS, own, piece), BF),
            pltpu.VMEM((CHIPS - 1, own, piece), BF),
            dma((blocks,)),
            dma((3,)),
            dma((CHIPS + ZS - 1,)),
            dma((CHIPS + ZS - 1,)),
            dma((imgs,)),
            dma((imgs,)),
            dma((imgs,)),
            dma((2 * imgs,)),
            dma((2 * imgs,)),
            dma((2 * imgs,)),
            dma((imgs,)),
            dma((imgs,)),
            dma((imgs,)),
            dma((imgs,)),
            dma((4 * imgs,)),
            dma((ZS + CHIPS,)),
            dma((ZS + CHIPS,)),
        ],
        compiler_params=pltpu.CompilerParams(
            collective_id=0, has_side_effects=True, vmem_limit_bytes=52 * 2**20
        ),
        name="exchange",
    )(tok, go, so, sp)
    gso_out, gt_out, gp_out = pl.pallas_call(
        settle,
        out_shape=(
            jax.ShapeDtypeStruct((own, blocks, lanes, width), BF),
            jax.ShapeDtypeStruct((imgs, toks, width), BF),
            jax.ShapeDtypeStruct((own, piece), F32),
        ),
        in_specs=[vmem] * 3,
        out_specs=(anywhere,) * 3,
        scratch_shapes=[
            pltpu.VMEM((own * lanes, own * lanes), BF),
            pltpu.VMEM((blocks, own, lanes, width), BF),
            dma((2 + blocks,)),
        ],
        compiler_params=pltpu.CompilerParams(vmem_limit_bytes=20 * 2**20),
        name="settle",
    )(gso, gt, gp)
    return (
        jnp.swapaxes(gt_out, 0, 1),
        gso_out.reshape(own, all_imgs, width),
        gp_out,
    )


def solution(mesh):
    return jax.shard_map(
        per_device,
        mesh=mesh,
        in_specs=(
            P(None, ("dp", "expert"), None),
            P(None, ("dp", "expert"), None),
            P("expert", "dp", None),
            P("expert", None),
        ),
        out_specs=(P(None, ("dp", "expert"), None), P("expert", "dp", None), P("expert", "dp")),
        check_vma=False,
    )
```

```python
import functools

import jax
import jax.numpy as jnp
from jax import lax
from jax.experimental import pallas as pl
from jax.experimental.pallas import tpu as pltpu
from jax.sharding import PartitionSpec as P

MESH = pl.DeviceIdType.MESH
BF = jnp.bfloat16
F32 = jnp.float32

ROWS, XS, CORES = 2, 4, 2
NEAR, ZS = 2, 4
CHIPS = ROWS * XS
STEPS = ((1, 0), (1, 2), (0, 1), (0, 3), (1, 1), (1, 3), (0, 2))
ORDER = tuple((r, x, c) for c in range(CORES) for r, x in STEPS) + ((0, 0, 1),)
NT = (((1,), (1,)), ((), ()))
TN = (((0,), (0,)), ((), ()))
NN = (((1,), (0,)), ((), ()))
KINDS = (0, 1, 2)
HELPER = ((1, 0), (0, 1), (0, 3))
PARTS = (
    (((0, 0), (0, 1), (0, 2), (0, 3)), ((0, 0), (1, 0), (0, 3), (1, 3)), ((0, 0), (1, 0), (0, 1), (1, 1))),
    (((0, 0), (0, 1), (0, 2), (0, 3)), ((0, 0), (1, 0), (0, 1), (1, 1)), ((0, 0), (1, 0), (0, 3), (1, 3))),
)
PIECES = 4
CLOSE = ((1, 0, 0), (0, 1, 0), (0, 3, 0), (0, 0, 1))
MIX = tuple(kind * 8 + k * CORES + dc for dc in range(CORES) for k in (3, 1, 2, 0) for kind in (0, 1))
BACK = tuple(tuple(tuple((k, of[k]) for k in (3, 1, 2, 0)) for of in kind) for kind in PARTS)


def back(at):
    return ((ROWS - at[0]) % ROWS, (XS - at[1]) % XS)


def add(a, b):
    return ((a[0] + b[0]) % ROWS, (a[1] + b[1]) % XS)


def dot(a, b, dims):
    return lax.dot_general(a, b, dims, preferred_element_type=F32)


def row_order(own, lanes, flip):
    n = own * lanes
    r = lax.broadcasted_iota(jnp.int32, (n, n), 0)
    c = lax.broadcasted_iota(jnp.int32, (n, n), 1)
    if flip:
        hit = c == (r % lanes) * own + r // lanes
    else:
        hit = c == (r % own) * lanes + r // own
    return jnp.where(hit, 1.0, 0.0).astype(BF)


def exchange(
    tok_hbm, go_hbm, so_hbm, sp_hbm,
    gso, gt, gp,
    tok, go, raw, send_a, slot_in, send_b, par, comb, low_w, low_s, gc_s, gc_r, gc_all, pp, perm,
    r1s, r1r, acc, r2s, r2r, r3s, r3r, r4s, r4r,
    so_sem, in_sem, par_s, par_r, go_s, go_r, as_sem, ar_sem, bs_sem, br_sem,
    low_ss, low_rs, gc_ss, gc_rs, own_sem, red_s, red_r, ready,
):
    imgs, width, tokens = tok.shape[0], tok.shape[2], tok.shape[1]
    blocks, own, lanes = raw.shape[0], so_hbm.shape[0], so_hbm.shape[2]
    slots = CHIPS * CORES * own
    half = slots // 2
    rounds = imgs // len(KINDS)
    d = lax.axis_index("dp")
    e = lax.axis_index("expert")
    row, x, c = e // (XS * CORES), (e // CORES) % XS, e % CORES
    chip = e // CORES
    near, z = d // ZS, d % ZS

    def chip_at(dr, dx):
        return ((row + dr) % ROWS) * XS + (x + dx) % XS

    def peer(dr, dx, dc):
        return chip_at(dr, dx) * CORES + (c + dc) % CORES

    def zpeer(k):
        return (near * ZS + (z + k) % ZS, e)

    side = ((1 - near) * ZS + z, e)
    partner = (d, peer(0, 0, 1))

    barrier = pltpu.get_barrier_semaphore()
    close = [(d, peer(*o)) for o in CLOSE]
    others = close + [zpeer(k) for k in range(1, ZS)] + [side]
    for dev in others:
        pl.semaphore_signal(barrier, inc=1, device_id=dev, device_id_type=MESH)

    def load_so(g):
        return pltpu.make_async_copy(so_hbm.at[:, g], raw.at[g], so_sem.at[g])

    sp_in = pltpu.make_async_copy(sp_hbm.at[z], par.at[chip, c, z], in_sem.at[0])
    go_in = pltpu.make_async_copy(go_hbm, go.at[pl.ds(0, imgs)], in_sem.at[1])
    tok_in = pltpu.make_async_copy(tok_hbm, tok, in_sem.at[2])
    sp_in.start()
    go_in.start()
    for g in range(blocks):
        load_so(g).start()
    tok_in.start()
    perm[...] = row_order(own, lanes, False)

    pl.semaphore_wait(barrier, len(others))

    def remote(src, dst, s, r, dev):
        return pltpu.make_async_remote_copy(
            src_ref=src, dst_ref=dst, send_sem=s, recv_sem=r, device_id=dev, device_id_type=MESH
        )

    def all_of(ref, sem):
        return pltpu.make_async_copy(ref, ref, sem)

    def par_row(i):
        r, dx = STEPS[i]
        piece = par.at[chip, c, z]
        return remote(piece, piece, par_s.at[i], par_r.at[i], (d, peer(r, dx, 0)))

    def par_z(k):
        piece = par.at[:, c, z]
        n = len(STEPS) + k - 1
        return remote(piece, piece, par_s.at[n], par_r.at[n], zpeer(k))

    def par_core():
        piece = par.at[:, c]
        n = len(STEPS) + ZS - 1
        return remote(piece, piece, par_s.at[n], par_r.at[n], partner)

    def helper(t):
        return (d, peer(*HELPER[t], 0))

    def home(t):
        return (d, peer(*back(HELPER[t]), 0))

    def send_go(q):
        rows = pl.ds(q * (tokens // PIECES), tokens // PIECES)
        for j in range(imgs):
            remote(
                go.at[j, rows], go.at[imgs + j, rows], go_s.at[j], go_r.at[j], helper(j % len(KINDS))
            ).start()

    go_in.wait()
    send_go(0)
    for i in range(len(CLOSE) - 1):
        for dev in close:
            pl.semaphore_signal(ready.at[i], inc=1, device_id=dev, device_id_type=MESH)
        pl.semaphore_wait(ready.at[i], len(close))
    sp_in.wait()
    for i in range(len(STEPS)):
        par_row(i).start()
    for q in range(1, PIECES):
        send_go(q)

    @pl.loop(0, blocks)
    def _(g):
        load_so(g).wait()
        block = raw.at[g].reshape(own * lanes, width)
        out = send_a.at[pl.ds(g * lanes, lanes)].reshape(own * lanes, width)
        for n in range(0, width, 256):
            out[:, n : n + 256] = dot(perm[...], block[:, n : n + 256], NN).astype(BF)

    def out_moves(j, t):
        for kind in range(2):
            for k, (dr, dx) in enumerate(PARTS[kind][t]):
                for dc in range(CORES):
                    at = back((dr, dx))
                    hr, hx = at if kind == 0 else add(at, back(HELPER[t]))
                    image = peer(hr, hx, dc) * imgs + j
                    yield kind, k, (*at, dc), send_a.at[image], slot_in.at[kind * imgs + j, k, c]

    def send_out(j, t, kinds):
        moves = list(out_moves(j, t))
        for i in MIX:
            kind, _, o, src, dst = moves[i]
            if kind not in kinds:
                continue
            w = kind * imgs + j
            if o == (0, 0, 0):
                pltpu.make_async_copy(src, dst, own_sem.at[w]).start()
            else:
                remote(src, dst, as_sem.at[j], ar_sem.at[w], (d, peer(*o))).start()

    def wait_out(w):
        all_of(slot_in.at[w].reshape(2 * len(PARTS[0][0]), own, width).at[pl.ds(0, 7)], ar_sem.at[w]).wait()
        all_of(send_a.at[0], own_sem.at[w]).wait()

    def send_back(kind, r, dcs):
        for dc in dcs:
            for i in range(4):
                for t in range(len(KINDS)):
                    j = r * len(KINDS) + t
                    hr, hx = (0, 0) if kind == 0 else back(HELPER[t])
                    w = kind * imgs + j
                    k, (dr, dx) = BACK[kind][t][i]
                    src, dst = send_b.at[w, k, (c + dc) % CORES], gso.at[peer(hr, hx, 0) * imgs + j]
                    if (dr, dx, dc) == (0, 0, 0):
                        pltpu.make_async_copy(src, dst, own_sem.at[2 * imgs + w]).start()
                    else:
                        remote(src, dst, bs_sem.at[w], br_sem.at[w], (d, peer(dr, dx, dc))).start()

    for t in range(len(KINDS)):
        send_out(t, t, (0, 1))

    for i in range(len(STEPS)):
        par_row(i).wait_recv()
    for k in range(1, ZS):
        par_z(k).start()
    for k in range(1, ZS):
        par_z(k).wait_recv()
    par_core().start()
    par_core().wait_recv()
    tok_in.wait()

    params = par.reshape(slots, width)

    def part_chips(kind, t):
        at = (0, 0) if kind == 0 else HELPER[t]
        return [chip_at(*add(at, p)) for p in PARTS[kind][t]]

    def send_low(j, t):
        return remote(low_s.at[j], low_w.at[imgs + j], low_ss.at[j], low_rs.at[j], helper(t))

    @pl.loop(0, rounds)
    def _(r):
        for t in range(len(KINDS)):
            j = r * len(KINDS) + t
            logits = dot(params[...], tok[j], NT)
            top = jnp.max(logits, axis=0, keepdims=True)
            raised = jnp.exp(logits - top)
            weight = raised / jnp.sum(raised, axis=0, keepdims=True)
            comb[j] = weight.reshape(CHIPS, CORES * own, tokens)
            for k, p in enumerate(part_chips(0, t)):
                low_w[j, k] = comb[j, p].astype(BF)
            for k, p in enumerate(part_chips(1, t)):
                low_s[j, k] = comb[j, p].astype(BF)
            if t > 0:
                send_low(j - 1, t - 1).start()
        send_low(r * len(KINDS) + len(KINDS) - 1, len(KINDS) - 1).start()

    for kind in (1, 0):
        for t in range(len(KINDS)):
            send_out(len(KINDS) + t, t, (kind,))

    def slot_grads(w):
        low = low_w[w].reshape(half, tokens)
        out = send_b.at[w].reshape(half, width)
        for n in range(0, width, 256):
            out[:, n : n + 256] = dot(low, go[w, :, n : n + 256], NN).astype(BF)

    @pl.loop(0, imgs)
    def _(j):
        slot_grads(j)

    def logit_dot(w):
        return dot(slot_in[w].reshape(half, width), go[w], NT).reshape(-1, CORES * own, tokens)

    def send_gc(j, t):
        return remote(gc_s.at[j], gc_r.at[j], gc_ss.at[j], gc_rs.at[j], home(t))

    @pl.loop(0, rounds)
    def _(r):
        for t in range(len(KINDS)):
            j = r * len(KINDS) + t
            all_of(low_w.at[imgs + j], low_rs.at[j]).wait()
            all_of(go.at[imgs + j], go_r.at[j]).wait()
            slot_grads(imgs + j)
            wait_out(imgs + j)
            gc_s[j] = logit_dot(imgs + j).astype(BF)
            if t > 0:
                send_gc(j - 1, t - 1).start()
        send_gc(r * len(KINDS) + len(KINDS) - 1, len(KINDS) - 1).start()

    for r in range(rounds):
        send_back(0, r, (0, 1))
    pp[...] = jnp.zeros_like(pp)

    @pl.loop(0, rounds)
    def _(r):
        for t in range(len(KINDS)):
            j = r * len(KINDS) + t
            wait_out(j)
            part = logit_dot(j)
            for k, p in enumerate(part_chips(0, t)):
                gc_all[p] = part[k]
            send_gc(j, t).wait_recv()
            for k, p in enumerate(part_chips(1, t)):
                gc_all[p] = gc_r[j, k].astype(F32)
            grad = gc_all[...].reshape(slots, tokens)
            weight = comb[j].reshape(slots, tokens)
            rowdot = jnp.sum(weight * grad, axis=0, keepdims=True)
            low = (weight * (grad - rowdot)).astype(BF)
            for n in range(0, width, 256):
                pp[:, n : n + 256] += dot(low, tok[j, :, n : n + 256], NN)
                gt[j, :, n : n + 256] = dot(low, params[:, n : n + 256], TN).astype(BF)

    share = pp.reshape(CHIPS, CORES, own, width)
    r1s[...] = share[:, 1 - c].astype(BF)
    over_core = remote(r1s, r1r, red_s.at[0], red_r.at[0], partner)
    send_back(1, 0, (0, 1))
    over_core.start()
    over_core.wait_recv()
    both = (share[:, c] + r1r[...].astype(F32)).reshape(CHIPS * own, width)
    piece = width // (NEAR * ZS)
    for n in range(NEAR):
        for k in range(ZS):
            m = (n * ZS + k) * piece
            acc[k, n] = both[:, m : m + piece]
    r2s[...] = acc[...].astype(BF)

    def over_z(k):
        return remote(r2s.at[(z + k) % ZS], r2r.at[k - 1], red_s.at[k], red_r.at[k], zpeer(k))

    for k in range(1, ZS):
        over_z(k).start()
    total = acc[z]
    for k in range(1, ZS):
        over_z(k).wait_recv()
        total = total + r2r[k - 1].astype(F32)
    acc[0] = total
    r3s[...] = acc[0, 1 - near].astype(BF)
    over_side = remote(r3s, r3r, red_s.at[ZS], red_r.at[ZS], side)
    over_side.start()
    send_back(1, 1, (0,))
    over_side.wait_recv()
    mine = (acc[0, near] + r3r[...].astype(F32)).reshape(CHIPS, own, piece)
    r4s[...] = mine.astype(BF)
    acc[1, 0] = mine.reshape(CHIPS * own, piece)

    def over_chips(i):
        p = peer(*STEPS[i], 0)
        return remote(r4s.at[p // CORES], r4r.at[i], red_s.at[ZS + 1 + i], red_r.at[ZS + 1 + i], (d, p))

    for i in range(len(STEPS)):
        over_chips(i).start()
    send_back(1, 1, (1,))
    owned = acc.at[1, 0].reshape(CHIPS, own, piece)[chip]
    for i in range(len(STEPS)):
        over_chips(i).wait_recv()
        owned = owned + r4r[i].astype(F32)
    gp[...] = owned

    for i in range(len(STEPS)):
        par_row(i).wait_send()
        over_chips(i).wait_send()
    for k in range(1, ZS):
        par_z(k).wait_send()
        over_z(k).wait_send()
    par_core().wait_send()
    over_core.wait_send()
    over_side.wait_send()

    @pl.loop(0, imgs)
    def _(j):
        all_of(go.at[j], go_s.at[j]).wait()
        all_of(low_s.at[j], low_ss.at[j]).wait()
        all_of(gc_s.at[j], gc_ss.at[j]).wait()
        all_of(send_a.at[pl.ds(0, 14)], as_sem.at[j]).wait()

    @pl.loop(0, 2 * imgs)
    def _(w):
        all_of(send_a.at[pl.ds(0, 7)], bs_sem.at[w]).wait()
        all_of(send_a.at[0], own_sem.at[2 * imgs + w]).wait()
        all_of(gso.at[pl.ds(0, 7)], br_sem.at[w]).wait()


def settle(gso, gt, gp, gso_out, gt_out, gp_out, perm, stage, sems):
    lanes, own = gso_out.shape[2], gso_out.shape[0]
    width = gso_out.shape[3]
    blocks = gso_out.shape[1]
    gt_copy = pltpu.make_async_copy(gt, gt_out, sems.at[0])
    gp_copy = pltpu.make_async_copy(gp, gp_out, sems.at[1])
    gt_copy.start()
    gp_copy.start()
    perm[...] = row_order(own, lanes, True)

    def put(g):
        return pltpu.make_async_copy(stage.at[g], gso_out.at[:, g], sems.at[2 + g])

    @pl.loop(0, blocks // 4)
    def _(h):
        for g in range(4):
            block = gso.at[pl.ds((h * 4 + g) * lanes, lanes)].reshape(own * lanes, width)
            out = stage.at[h * 4 + g].reshape(own * lanes, width)
            out[...] = dot(perm[...], block[...], NN).astype(BF)
        for g in range(4):
            put(h * 4 + g).start()

    @pl.loop(0, blocks)
    def _(g):
        put(g).wait()

    gt_copy.wait()
    gp_copy.wait()


def per_device(tokens, grad_out, slot_out, slot_params):
    toks, imgs, width = tokens.shape
    own, all_imgs, _ = slot_out.shape
    lanes = 8
    blocks = all_imgs // lanes
    slots = CHIPS * CORES * own
    tok = jnp.swapaxes(tokens, 0, 1)
    go = jnp.swapaxes(grad_out, 0, 1)
    so = slot_out.reshape(own, blocks, lanes, width)
    sp = slot_params.reshape(ZS, own // ZS, width)
    piece = width // (NEAR * ZS)
    anywhere = pl.BlockSpec(memory_space=pl.ANY)
    vmem = pl.BlockSpec(memory_space=pltpu.VMEM)
    dma = pltpu.SemaphoreType.DMA
    gso, gt, gp = pl.pallas_call(
        exchange,
        out_shape=(
            pltpu.VMEM((all_imgs, own, width), BF),
            pltpu.VMEM((imgs, toks, width), BF),
            pltpu.VMEM((own, piece), F32),
        ),
        in_specs=[anywhere] * 4,
        out_specs=(vmem, vmem, vmem),
        scratch_shapes=[
            pltpu.VMEM((imgs, toks, width), BF),
            pltpu.VMEM((2 * imgs, toks, width), BF),
            pltpu.VMEM((blocks, own, lanes, width), BF),
            pltpu.VMEM((all_imgs, own, width), BF),
            pltpu.VMEM((2 * imgs, 4, CORES, own, width), BF),
            pltpu.VMEM((2 * imgs, 4, CORES, own, width), BF),
            pltpu.VMEM((CHIPS, CORES, ZS, own // ZS, width), BF),
            pltpu.VMEM((imgs, CHIPS, CORES * own, toks), F32),
            pltpu.VMEM((2 * imgs, 4, CORES * own, toks), BF),
            pltpu.VMEM((imgs, 4, CORES * own, toks), BF),
            pltpu.VMEM((imgs, 4, CORES * own, toks), BF),
            pltpu.VMEM((imgs, 4, CORES * own, toks), BF),
            pltpu.VMEM((CHIPS, CORES * own, toks), F32),
            pltpu.VMEM((slots, width), F32),
            pltpu.VMEM((own * lanes, own * lanes), BF),
            pltpu.VMEM((CHIPS, own, width), BF),
            pltpu.VMEM((CHIPS, own, width), BF),
            pltpu.VMEM((ZS, NEAR, CHIPS * own, piece), F32),
            pltpu.VMEM((ZS, NEAR, CHIPS * own, piece), BF),
            pltpu.VMEM((ZS - 1, NEAR, CHIPS * own, piece), BF),
            pltpu.VMEM((CHIPS * own, piece), BF),
            pltpu.VMEM((CHIPS * own, piece), BF),
            pltpu.VMEM((CHIPS, own, piece), BF),
            pltpu.VMEM((CHIPS - 1, own, piece), BF),
            dma((blocks,)),
            dma((3,)),
            dma((CHIPS + ZS - 1,)),
            dma((CHIPS + ZS - 1,)),
            dma((imgs,)),
            dma((imgs,)),
            dma((imgs,)),
            dma((2 * imgs,)),
            dma((2 * imgs,)),
            dma((2 * imgs,)),
            dma((imgs,)),
            dma((imgs,)),
            dma((imgs,)),
            dma((imgs,)),
            dma((4 * imgs,)),
            dma((ZS + CHIPS,)),
            dma((ZS + CHIPS,)),
            pltpu.SemaphoreType.REGULAR((len(CLOSE) - 1,)),
        ],
        compiler_params=pltpu.CompilerParams(
            collective_id=0, has_side_effects=True, vmem_limit_bytes=52 * 2**20
        ),
        name="exchange",
    )(tok, go, so, sp)
    gso_out, gt_out, gp_out = pl.pallas_call(
        settle,
        out_shape=(
            jax.ShapeDtypeStruct((own, blocks, lanes, width), BF),
            jax.ShapeDtypeStruct((imgs, toks, width), BF),
            jax.ShapeDtypeStruct((own, piece), F32),
        ),
        in_specs=[vmem] * 3,
        out_specs=(anywhere,) * 3,
        scratch_shapes=[
            pltpu.VMEM((own * lanes, own * lanes), BF),
            pltpu.VMEM((blocks, own, lanes, width), BF),
            dma((2 + blocks,)),
        ],
        compiler_params=pltpu.CompilerParams(vmem_limit_bytes=20 * 2**20),
        name="settle",
    )(gso, gt, gp)
    return (
        jnp.swapaxes(gt_out, 0, 1),
        gso_out.reshape(own, all_imgs, width),
        gp_out,
    )


def solution(mesh):
    return jax.shard_map(
        per_device,
        mesh=mesh,
        in_specs=(
            P(None, ("dp", "expert"), None),
            P(None, ("dp", "expert"), None),
            P("expert", "dp", None),
            P("expert", None),
        ),
        out_specs=(P(None, ("dp", "expert"), None), P("expert", "dp", None), P("expert", "dp")),
        check_vma=False,
    )
```
